32 devices in a mesh: rep: 2 (over z, core), dp: 16 (over x, y).
Axes of the slice: x: 4, y: 4, z: 1, core: 2. Of those that a mesh axis runs over, the one named last changes fastest.
The devices are a block of a 4x4x8 slice.
Arguments:
- x: bfloat16 [32, 2048, 1024], P(('rep', 'dp')), parts along dimension 0
- dy: bfloat16 [32, 2048, 1024], P(('rep', 'dp')), parts along dimension 0
- w_gate: bfloat16 [2, 1024, 4096], replicated
- w_up: bfloat16 [2, 1024, 4096], replicated
- w_down: bfloat16 [2, 4096, 1024], replicated
- m_w_gate: float32 [2, 1024, 4096], P(None, 'dp')
- m_w_up: float32 [2, 1024, 4096], P(None, 'dp')
- m_w_down: float32 [2, 4096, 1024], P(None, 'dp')
- v_w_gate: float32 [2, 1024, 4096], P(None, 'dp')
- v_w_up: float32 [2, 1024, 4096], P(None, 'dp')
- v_w_down: float32 [2, 4096, 1024], P(None, 'dp')
Outputs:
- output 1: bfloat16 [4, 1024, 4096], P('rep'), parts along dimension 0
- output 2: bfloat16 [4, 1024, 4096], P('rep'), parts along dimension 0
- output 3: bfloat16 [4, 4096, 1024], P('rep'), parts along dimension 0
- output 4: float32 [4, 1024, 4096], P('rep', 'dp'), parts along dimension 0
- output 5: float32 [4, 1024, 4096], P('rep', 'dp'), parts along dimension 0
- output 6: float32 [4, 4096, 1024], P('rep', 'dp'), parts along dimension 0
- output 7: float32 [4, 1024, 4096], P('rep', 'dp'), parts along dimension 0
- output 8: float32 [4, 1024, 4096], P('rep', 'dp'), parts along dimension 0
- output 9: float32 [4, 4096, 1024], P('rep', 'dp'), parts along dimension 0
There are 2 independent parts. The reference program is written for one: setup_inputs(seed, part) draws one part's arguments, and reference() takes and returns one part's arrays. A program takes and returns all parts, laid end to end along the dimension named above; an argument that names none is the same for every part.
All inputs are finite; a program needn't handle non-finite values.
Results may differ from the reference program's by a relative error of at most 0.022.
Values are sent between devices in bfloat16 or wider.
A program may use at most 768 MiB of HBM per device.

```python
import jax
import jax.numpy as jnp
from jax import lax

SEQUENCES = 16
TOKENS = 2048
D = 1024
FF = 4096
LAYERS = 2
NAMES = ("w_gate", "w_up", "w_down")
SHAPES = {"w_gate": (LAYERS, D, FF), "w_up": (LAYERS, D, FF), "w_down": (LAYERS, FF, D)}


def bump(key, n, height):
    away = (jnp.arange(n, dtype=jnp.int32) - jax.random.randint(key, (), 0, n, jnp.int32)) % n
    return jnp.where(away < n // 8, height, 1.0)


def together(key, own, strength):
    shared = jax.random.normal(key, own.shape[1:], jnp.float32)
    return (own + strength * shared) * lax.rsqrt(1 + strength * strength)


def setup_inputs(seed: int = 0, part: int = 0) -> dict:
    kx, kdy, ka, kb, kz, kf, kh, kl, *keys = jax.random.split(jax.random.key(seed), 8 + 3 * len(NAMES))
    kx, kdy, ka, kb = (jax.random.fold_in(k, part) for k in (kx, kdy, ka, kb))
    kw, km, kv = (keys[i::3] for i in range(3))
    shape = (SEQUENCES, TOKENS, D)
    much_x, much_dy = jax.random.uniform(kz, (2,), jnp.float32, 0.0, 1.0)
    loud = 2.0 ** jax.random.uniform(jax.random.fold_in(kz, 1), (), jnp.float32, -1.0, 2.0)
    layers = 2.0 ** jax.random.uniform(kl, (LAYERS, 1, 1), jnp.float32, -1.0, 1.0)
    x = together(ka, jax.random.normal(kx, shape, jnp.float32), much_x) * bump(kf, D, 4.0)
    dy = together(kb, jax.random.normal(kdy, shape, jnp.float32), much_dy)
    drawn = {"x": x.astype(jnp.bfloat16), "dy": (loud * dy * (SEQUENCES * TOKENS) ** -0.5).astype(jnp.bfloat16)}
    for key, name in zip(kw, NAMES, strict=True):
        w = jax.random.normal(key, SHAPES[name], jnp.float32) * SHAPES[name][1] ** -0.5
        drawn[name] = (w * {"w_gate": 1.0, "w_up": bump(kh, FF, 4.0), "w_down": layers}[name]).astype(jnp.bfloat16)
    for key, name in zip(km, NAMES, strict=True):
        drawn[f"m_{name}"] = 0.1 * jax.random.normal(key, SHAPES[name], jnp.float32)
    for key, name in zip(kv, NAMES, strict=True):
        drawn[f"v_{name}"] = jax.random.uniform(key, SHAPES[name], jnp.float32, 0.005, 0.015)
    return drawn


def matmul(a, w):
    return jnp.dot(a, w, preferred_element_type=jnp.float32).astype(jnp.bfloat16)


def normed(h):
    wide = h.astype(jnp.float32)
    scale = lax.rsqrt(jnp.mean(wide**2, -1, keepdims=True) + 1e-6)
    return (wide * scale).astype(jnp.bfloat16)


def layer(h, w):
    a = normed(h)
    gate = jnp.dot(a, w["w_gate"], preferred_element_type=jnp.float32)
    up = jnp.dot(a, w["w_up"], preferred_element_type=jnp.float32)
    return h + matmul((jax.nn.silu(gate) * up).astype(jnp.bfloat16), w["w_down"])


def adamw(w, m, v, g):
    m = 0.9 * m + 0.1 * g
    v = 0.95 * v + 0.05 * g * g
    step = m * lax.rsqrt(v + 1e-8) + 0.1 * w
    return (w - 0.02 * step).astype(jnp.bfloat16), m, v


def stack(weights, h):
    return lax.scan(lambda h, w: (layer(h, w), None), h, weights)[0]


def reference(x, dy, w_gate, w_up, w_down, m_w_gate, m_w_up, m_w_down, v_w_gate, v_w_up, v_w_down):
    weights = dict(zip(NAMES, (w_gate, w_up, w_down), strict=True))

    def take(so_far, sequence):
        h, by_y = sequence
        _, back = jax.vjp(lambda w: stack(w, h), weights)
        return jax.tree.map(lambda total, term: total + term.astype(jnp.float32), so_far, back(by_y)[0]), None

    none_yet = {name: jnp.zeros(w.shape, jnp.float32) for name, w in weights.items()}
    by_weights, _ = lax.scan(take, none_yet, (x, dy))
    gradients = [by_weights[name].astype(jnp.bfloat16).astype(jnp.float32) for name in NAMES]
    new = [
        adamw(w.astype(jnp.float32), m, v, g)
        for w, m, v, g in zip((w_gate, w_up, w_down), (m_w_gate, m_w_up, m_w_down), (v_w_gate, v_w_up, v_w_down), gradients, strict=True)
    ]
    return tuple(one[which] for which in range(3) for one in new)
```

```python
import functools
import math

import jax
import jax.numpy as jnp
from jax import lax
from jax.experimental import pallas as pl
from jax.experimental.pallas import tpu as pltpu
from jax.sharding import PartitionSpec as P

F32, BF16 = jnp.float32, jnp.bfloat16
MESH = pl.DeviceIdType.MESH
VMEM_LIMIT = 64 * 1024 * 1024 - 128 * 1024
FLOWS = 4
HOPS = 3
ROW_TILES = 4


def mm(a, b, dims=((1,), (0,))):
    return lax.dot_general(a, b, (dims, ((), ())), preferred_element_type=F32)


def scale_of(wide):
    return lax.rsqrt(jnp.mean(wide**2, -1, keepdims=True) + 1e-6)


def adamw(w, m, v, g):
    m = 0.9 * m + 0.1 * g
    v = 0.95 * v + 0.05 * g * g
    step = m * lax.rsqrt(v + 1e-8) + 0.1 * w
    return (w - 0.02 * step).astype(BF16), m, v


class Sizes:
    def __init__(self, tokens, d, ff, layers, group):
        self.tokens, self.d, self.ff, self.layers, self.group = tokens, d, ff, layers, group
        self.side = math.isqrt(group)
        self.rows = d // group
        self.quarters = ff // group // self.rows
        assert self.quarters == FLOWS and self.side == HOPS + 1
        self.cols = d // 4
        self.fb = 2 * self.cols
        self.gu_units = ff // self.fb
        self.d_units = d // self.cols
        self.per_layer = self.gu_units + self.d_units
        self.units = layers * self.per_layer


def step_kernel(
    z,
    h1_in, a1_in, a0_in, dy_in, wg_in, wu_in, wd_in, mg_in, mu_in, md_in, vg_in, vu_in, vd_in,
    w_out, g_out, dgu_hbm, pt_hbm,
    a, at, d, da, wg, wu, wd, dgu, pt, grads,
    hrecv, hsend, hsum, lrecv, lsend, w_new, g_own, w_old, m_old, v_old,
    hs, hr, ls, lr, als, alr, ahs, ahr, own_sem, g_sem, adam_sem, w_sem, in_sem, dgu_sem, pt_sem,
):
    side, rows, cols, fb = z.side, z.rows, z.cols, z.fb
    rep, me = lax.axis_index("rep"), lax.axis_index("dp")
    cx, cy = me // side, me % side
    first = [cx, cx, cy, cy]
    second = [cy, cy, cx, cx]
    way = [1, -1, 1, -1]

    def device(x, y):
        return (rep, ((x + side) % side) * side + (y + side) % side)

    def next_on_first(f):
        return device(cx + way[f], cy) if f < 2 else device(cx, cy + way[f])

    def next_on_second(f):
        return device(cx, cy + way[f]) if f < 2 else device(cx + way[f], cy)

    def behind(at_, f, n):
        return (at_ - way[f] * n + 2 * side) % side

    def remote(src, dst, send, recv, target):
        return pltpu.make_async_remote_copy(src, dst, send, recv, device_id=target, device_id_type=MESH)

    def h_copy(u, s, f):
        par = u % 2
        src = grads.at[u % 3, f, pl.ds(side * behind(first[f], f, 1), side)] if s == 0 else hsend.at[par, s - 1, f]
        return remote(src, hrecv.at[par, s, f], hs.at[par, s, f], hr.at[par, s, f], next_on_first(f))

    def l_copy(u, s, f):
        par = u % 2
        return remote(lsend.at[par, s, f], lrecv.at[par, s, f], ls.at[par, s, f], lr.at[par, s, f], next_on_second(f))

    def al_copy(u, s, f):
        par = u % 2
        place = side * first[f] + behind(second[f], f, s)
        dst = w_out.at[u, f, place]
        src = w_new.at[par, f] if s == 0 else dst
        return remote(src, dst, als.at[par, s, f], alr.at[par, s, f], next_on_second(f))

    def ah_copy(u, s, f):
        par = u % 2
        dst = w_out.at[u, f, pl.ds(side * behind(first[f], f, s), side)]
        return remote(dst, dst, ahs.at[par, s, f], ahr.at[par, s, f], next_on_first(f))

    def own_copy(u, f):
        return pltpu.make_async_copy(w_new.at[u % 2, f], w_out.at[u, f, side * first[f] + second[f]], own_sem.at[u % 2, f])

    def g_copy(u):
        return pltpu.make_async_copy(g_own.at[u % 2], g_out.at[u], g_sem.at[u % 2])

    def place_of(u):
        return z.layers - 1 - u // z.per_layer, u % z.per_layer

    def adam_loads(u, start):
        layer, k = place_of(u) if start else (0, 0)

        def go(copies):
            for c in copies:
                c.start()

        def copies_gu():
            c0 = pl.multiple_of(k * fb, fb)
            r0 = pl.multiple_of(me * rows, rows)
            out = []
            for f in range(FLOWS):
                col = pl.ds(c0 + (f % 2) * cols, cols)
                w_, m_, v_ = ((wg_in, mg_in, vg_in), (wu_in, mu_in, vu_in))[f // 2]
                out.append(pltpu.make_async_copy(w_.at[layer, pl.ds(r0, rows), col], w_old.at[f], adam_sem.at[0, f]))
                out.append(pltpu.make_async_copy(m_.at[layer, :, col], m_old.at[f], adam_sem.at[1, f]))
                out.append(pltpu.make_async_copy(v_.at[layer, :, col], v_old.at[f], adam_sem.at[2, f]))
            return out

        def copies_d():
            col = pl.ds(pl.multiple_of((k - z.gu_units) * cols, cols), cols)
            out = []
            for f in range(FLOWS):
                r0 = pl.multiple_of((me * FLOWS + f) * rows, rows)
                out.append(pltpu.make_async_copy(wd_in.at[layer, pl.ds(r0, rows), col], w_old.at[f], adam_sem.at[0, f]))
                out.append(pltpu.make_async_copy(md_in.at[layer, pl.ds(f * rows, rows), col], m_old.at[f], adam_sem.at[1, f]))
                out.append(pltpu.make_async_copy(vd_in.at[layer, pl.ds(f * rows, rows), col], v_old.at[f], adam_sem.at[2, f]))
            return out

        if start:
            pl.when(k < z.gu_units)(lambda: go(copies_gu()))
            pl.when(k >= z.gu_units)(lambda: go(copies_d()))
        else:
            for c in copies_gu():
                c.wait()

    def both(x, y):
        return x.astype(F32) + y.astype(F32)

    def h_hop(u, s):
        par, slot = u % 2, u % 3
        if s:
            for f in range(FLOWS):
                h_copy(u, s - 1, f).wait_recv()
                mine = grads[slot, f, pl.ds(side * behind(first[f], f, s + 1), side)]
                hsend[par, s - 1, f] = both(hrecv[par, s - 1, f], mine).astype(BF16)
        for f in range(FLOWS):
            h_copy(u, s, f).start()
            if s == HOPS - 1:
                h_copy(u, 0, f).wait_send()

    def h_end_l_start(u):
        par, slot = u % 2, u % 3
        for f in range(FLOWS):
            h_copy(u, HOPS - 1, f).wait_recv()
            hsum[par, f] = both(hrecv[par, HOPS - 1, f], grads[slot, f, pl.ds(side * first[f], side)])
            lsend[par, 0, f] = hsum[par, f, behind(second[f], f, 1)].astype(BF16)
        for f in range(FLOWS):
            l_copy(u, 0, f).start()
        for f in range(FLOWS):
            for s in range(1, HOPS):
                h_copy(u, s, f).wait_send()

    def l_hop(u, s):
        par = u % 2
        for f in range(FLOWS):
            l_copy(u, s - 1, f).wait_recv()
            lsend[par, s, f] = both(lrecv[par, s - 1, f], hsum[par, f, behind(second[f], f, s + 1)]).astype(BF16)
        for f in range(FLOWS):
            l_copy(u, s, f).start()

    def l_end_al_start(u):
        par = u % 2
        adam_loads(u, False)
        for f in range(FLOWS):
            l_copy(u, HOPS - 1, f).wait_recv()
            g = both(lrecv[par, HOPS - 1, f], hsum[par, f, second[f]]).astype(BF16)
            g_own[par, f] = g
            w_new[par, f] = adamw(w_old[f].astype(F32), m_old[f], v_old[f], g.astype(F32))[0]
        for f in range(FLOWS):
            al_copy(u, 0, f).start()
            own_copy(u, f).start()
        g_copy(u).start()
        for f in range(FLOWS):
            for s in range(HOPS):
                l_copy(u, s, f).wait_send()

    def al_hop(u, s):
        for f in range(FLOWS):
            al_copy(u, s - 1, f).wait_recv()
            al_copy(u, s, f).start()

    def al_end_ah_start(u):
        for f in range(FLOWS):
            al_copy(u, HOPS - 1, f).wait_recv()
            own_copy(u, f).wait()
            ah_copy(u, 0, f).start()
        for f in range(FLOWS):
            for s in range(HOPS):
                al_copy(u, s, f).wait_send()
        g_copy(u).wait()

    def ah_hop(u, s):
        for f in range(FLOWS):
            ah_copy(u, s - 1, f).wait_recv()
            ah_copy(u, s, f).start()

    def ah_end(u):
        for f in range(FLOWS):
            ah_copy(u, HOPS - 1, f).wait_recv()
            for s in range(HOPS):
                ah_copy(u, s, f).wait_send()

    def if_unit(u, step):
        pl.when((u >= 0) & (u < z.units))(lambda: step(u))

    def slot_0(h):
        if_unit(h, lambda u: h_hop(u, 0))
        if_unit(h - 8, ah_end)
        if_unit(h - 6, al_end_ah_start)
        if_unit(h - 4, l_end_al_start)
        if_unit(h - 2, h_end_l_start)

    def slot_1(h):
        if_unit(h - 1, lambda u: h_hop(u, 2))
        if_unit(h - 3, lambda u: l_hop(u, 2))
        if_unit(h - 5, lambda u: al_hop(u, 2))
        if_unit(h - 7, lambda u: ah_hop(u, 2))
        if_unit(h - 3, lambda u: adam_loads(u, True))

    def slot_2(h):
        if_unit(h, lambda u: h_hop(u, 1))
        if_unit(h - 2, lambda u: l_hop(u, 1))
        if_unit(h - 4, lambda u: al_hop(u, 1))
        if_unit(h - 6, lambda u: ah_hop(u, 1))

    tile = z.tokens // ROW_TILES

    def rows_of(t, size):
        return pl.ds(pl.multiple_of(t * size, size), size)

    def weight_loads(layer, j, buf, with_down):
        cols_j = pl.ds(pl.multiple_of(j * fb, fb), fb)
        out = [
            pltpu.make_async_copy(wg_in.at[layer, :, cols_j], wg.at[buf], w_sem.at[buf, 0]),
            pltpu.make_async_copy(wu_in.at[layer, :, cols_j], wu.at[buf], w_sem.at[buf, 1]),
        ]
        if with_down:
            out.append(pltpu.make_async_copy(wd_in.at[layer, cols_j, :], wd.at[buf], w_sem.at[buf, 2]))
        return out

    def backward_tile(t, buf):
        r = rows_of(t, tile)
        a_t = a[r, :]
        gate = mm(a_t, wg[buf])
        up = mm(a_t, wu[buf])
        dp = mm(d[r, :], wd[buf], ((1,), (1,))).astype(BF16).astype(F32)
        sig = jax.nn.sigmoid(gate)
        silu = gate * sig
        pt[0, :, r] = (silu * up).astype(BF16).T
        dgu[0, r, pl.ds(fb, fb)] = (dp * silu).astype(BF16)
        dgu[0, r, pl.ds(0, fb)] = (dp * up * (sig * (1 + gate * (1 - sig)))).astype(BF16)

    def keep_copies(j):
        return [
            pltpu.make_async_copy(pt.at[0], pt_hbm.at[j], pt_sem.at[0]),
            pltpu.make_async_copy(dgu.at[0], dgu_hbm.at[j], dgu_sem.at[0]),
        ]

    def store_block(slot, f, dev, value):
        x, y = dev // side, dev % side
        grads[slot, f, x * side + y if f < 2 else y * side + x] = value

    def gu_grads(m, slot):
        half = z.d // 2
        out = mm(at[rows_of(m, half), :], dgu[0]).astype(BF16)
        for n in range(z.group // 2):
            for f in range(FLOWS):
                store_block(slot, f, m * (z.group // 2) + n, out[n * rows : (n + 1) * rows, f * cols : (f + 1) * cols])

    def d_grads(t, i, slot):
        buf = t % 2
        pltpu.make_async_copy(pt_hbm.at[t], pt.at[buf], pt_sem.at[buf]).wait()
        out = mm(pt[buf], d[:, rows_of(i, cols)]).astype(BF16)
        devices = z.group // z.gu_units
        for n in range(devices):
            for f in range(FLOWS):
                r0 = (n * FLOWS + f) * rows
                store_block(slot, f, t * devices + n, out[r0 : r0 + rows])

        @pl.when(t + 2 < z.gu_units)
        def _():
            pltpu.make_async_copy(pt_hbm.at[t + 2], pt.at[buf], pt_sem.at[buf]).start()

    def d_first_loads():
        for t in range(2):
            pltpu.make_async_copy(pt_hbm.at[t], pt.at[t], pt_sem.at[t]).start()

    def da_tile(t, buf, fresh):
        r = rows_of(t, tile)
        part = mm(dgu[buf, r, pl.ds(0, fb)], wg[buf], ((1,), (1,))) + mm(dgu[buf, r, pl.ds(fb, fb)], wu[buf], ((1,), (1,)))

        @pl.when(fresh)
        def _():
            da[r, :] = part

        @pl.when(jnp.logical_not(fresh))
        def _():
            da[r, :] = da[r, :] + part

    def loop(lo, hi, body):
        lax.fori_loop(lo, hi, lambda i, c: (body(i), c)[1], 0)

    norm_tile = z.tokens // 16

    def norm_backward(t):
        r = rows_of(t, norm_tile)
        wide = a[r, :].astype(F32)
        scale = scale_of(wide)
        by_a = da[r, :].astype(BF16).astype(F32)
        inner = jnp.mean(by_a * wide, -1, keepdims=True)
        d[r, :] = both(d[r, :], (scale * by_a - wide * (scale**3 * inner)).astype(BF16)).astype(BF16)

    def transpose_tile(t):
        r = rows_of(t, norm_tile)
        at[:, r] = a[r, :].T

    last = z.layers - 1
    n_gu, n_d = z.gu_units, z.d_units
    a_end = n_gu - 1
    c_end = a_end + n_d
    a2_end = c_end + n_gu
    c2_end = a2_end + n_d
    per_c = n_gu // n_d

    def gu_index(h):
        return jnp.where(h < a_end, last, 0), jnp.where(h < a_end, h + 1, h - c_end)

    def piece_1(h):
        is_gu = (h < a_end) | ((h >= c_end) & (h < a2_end))
        is_d = ((h >= a_end) & (h < c_end)) | ((h >= a2_end) & (h < c2_end))
        layer, j = gu_index(h)

        @pl.when(h == c_end)
        def _():
            cp = pltpu.make_async_copy(a0_in, a, in_sem.at[0])
            cp.wait()
            loop(0, 16, transpose_tile)

        @pl.when(is_gu)
        def _():
            for c in weight_loads(layer, j, j % 2, True):
                c.wait()

            @pl.when(j + 1 < n_gu)
            def _():
                for c in weight_loads(layer, j + 1, (j + 1) % 2, True):
                    c.start()

            loop(0, ROW_TILES // 2, lambda t: backward_tile(t, j % 2))

        @pl.when((h >= a_end) & (h < c_end))
        def _():
            for b in range(per_c):
                blk = (h - a_end) * per_c + b
                for c in weight_loads(last, blk, b, False):
                    c.start()
                pltpu.make_async_copy(dgu_hbm.at[blk], dgu.at[b], dgu_sem.at[b]).start()

        @pl.when(h == a_end)
        def _():
            pltpu.make_async_copy(h1_in, a, in_sem.at[0]).start()

        @pl.when(is_d)
        def _():
            i = jnp.where(h < c_end, h - a_end, h - a2_end)
            d_first_loads()
            loop(0, n_gu // 2, lambda t: d_grads(t, i, (h + 1) % 3))

    def da_block(h, b):
        blk = (h - a_end) * per_c + b
        for c in weight_loads(last, blk, b, False):
            c.wait()
        pltpu.make_async_copy(dgu_hbm.at[blk], dgu.at[b], dgu_sem.at[b]).wait()
        loop(0, ROW_TILES, lambda t: da_tile(t, b, blk == 0))

    def piece_2(h):
        is_gu = (h < a_end) | ((h >= c_end) & (h < a2_end))
        is_d = ((h >= a_end) & (h < c_end)) | ((h >= a2_end) & (h < c2_end))
        layer, j = gu_index(h)

        @pl.when(is_gu)
        def _():
            loop(ROW_TILES // 2, ROW_TILES, lambda t: backward_tile(t, j % 2))

        @pl.when(is_d)
        def _():
            i = jnp.where(h < c_end, h - a_end, h - a2_end)
            loop(n_gu // 2, n_gu, lambda t: d_grads(t, i, (h + 1) % 3))

        @pl.when((h >= a_end) & (h < c_end))
        def _():
            da_block(h, 0)

    def piece_3(h):
        is_gu = (h < a_end) | ((h >= c_end) & (h < a2_end))
        layer, j = gu_index(h)

        @pl.when(is_gu)
        def _():
            for c in keep_copies(j):
                c.start()
            loop(0, 2, lambda m: gu_grads(m, (h + 1) % 3))
            for c in keep_copies(j):
                c.wait()

        @pl.when((h >= a_end) & (h < c_end))
        def _():
            for b in range(1, per_c):
                da_block(h, b)

        @pl.when(h == c_end - 1)
        def _():
            pltpu.make_async_copy(h1_in, a, in_sem.at[0]).wait()
            loop(0, 16, norm_backward)
            pltpu.make_async_copy(a0_in, a, in_sem.at[0]).start()
            for c in weight_loads(0, 0, 0, True):
                c.start()

    first_loads = [pltpu.make_async_copy(a1_in, a, in_sem.at[0]), pltpu.make_async_copy(dy_in, d, in_sem.at[1])]
    for c in first_loads + weight_loads(last, 0, 0, True) + weight_loads(last, 1, 1, True):
        c.start()
    barrier = pltpu.get_barrier_semaphore()
    for f in range(FLOWS):
        pl.semaphore_signal(barrier, inc=1, device_id=next_on_first(f), device_id_type=MESH)
    for c in first_loads + weight_loads(last, 0, 0, True):
        c.wait()
    loop(0, 16, transpose_tile)
    loop(0, ROW_TILES, lambda t: backward_tile(t, 0))
    for c in keep_copies(0):
        c.start()
    loop(0, 2, lambda m: gu_grads(m, 0))
    for c in keep_copies(0):
        c.wait()
    pl.semaphore_wait(barrier, FLOWS)

    def half_step(h):
        slot_0(h)
        piece_1(h)
        slot_1(h)
        piece_2(h)
        slot_2(h)
        piece_3(h)

    loop(0, z.units + 8, half_step)


def train_kernel_call(z, h1, a1, a0, dy, weights, moments):
    side, rows, cols, fb = z.side, z.rows, z.cols, z.fb
    dma = pltpu.SemaphoreType.DMA
    hbm = pl.BlockSpec(memory_space=pl.ANY)
    out_shape = (
        jax.ShapeDtypeStruct((z.units, FLOWS, z.group, rows, cols), BF16),
        jax.ShapeDtypeStruct((z.units, FLOWS, rows, cols), BF16),
        jax.ShapeDtypeStruct((z.gu_units, z.tokens, 2 * fb), BF16),
        jax.ShapeDtypeStruct((z.gu_units, fb, z.tokens), BF16),
    )
    scratch = [
        pltpu.VMEM((z.tokens, z.d), BF16),
        pltpu.VMEM((z.d, z.tokens), BF16),
        pltpu.VMEM((z.tokens, z.d), BF16),
        pltpu.VMEM((z.tokens, z.d), F32),
        pltpu.VMEM((2, z.d, fb), BF16),
        pltpu.VMEM((2, z.d, fb), BF16),
        pltpu.VMEM((2, fb, z.d), BF16),
        pltpu.VMEM((2, z.tokens, 2 * fb), BF16),
        pltpu.VMEM((2, fb, z.tokens), BF16),
        pltpu.VMEM((3, FLOWS, z.group, rows, cols), BF16),
        pltpu.VMEM((2, HOPS, FLOWS, side, rows, cols), BF16),
        pltpu.VMEM((2, HOPS - 1, FLOWS, side, rows, cols), BF16),
        pltpu.VMEM((2, FLOWS, side, rows, cols), F32),
        pltpu.VMEM((2, HOPS, FLOWS, rows, cols), BF16),
        pltpu.VMEM((2, HOPS, FLOWS, rows, cols), BF16),
        pltpu.VMEM((2, FLOWS, rows, cols), BF16),
        pltpu.VMEM((2, FLOWS, rows, cols), BF16),
        pltpu.VMEM((FLOWS, rows, cols), BF16),
        pltpu.VMEM((FLOWS, rows, cols), F32),
        pltpu.VMEM((FLOWS, rows, cols), F32),
        *[dma((2, HOPS, FLOWS)) for _ in range(8)],
        dma((2, FLOWS)),
        dma((2,)),
        dma((3, FLOWS)),
        dma((2, 3)),
        dma((2,)),
        dma((2,)),
        dma((2,)),
    ]
    return pl.pallas_call(
        functools.partial(step_kernel, z),
        out_shape=out_shape,
        in_specs=[hbm] * 13,
        out_specs=(hbm,) * 4,
        scratch_shapes=scratch,
        name="train_step",
        compiler_params=pltpu.CompilerParams(collective_id=0, has_side_effects=True, vmem_limit_bytes=VMEM_LIMIT),
    )(h1, a1, a0, dy, *weights, *moments)


def unpack_gu_kernel(z, w_ref, g_ref, mg_ref, mu_ref, vg_ref, vu_ref, wg_out, wu_out, mg_out, mu_out, vg_out, vu_out):
    side, rows, cols = z.side, z.rows, z.cols
    for f in range(FLOWS):
        out = (wg_out, wu_out)[f // 2]
        col = pl.ds((f % 2) * cols, cols)
        for n in range(z.group):
            x, y = n // side, n % side
            out[0, pl.ds(n * rows, rows), col] = w_ref[0, f, n if f < 2 else y * side + x]
        m_ref, v_ref, m_out, v_out = ((mg_ref, vg_ref, mg_out, vg_out), (mu_ref, vu_ref, mu_out, vu_out))[f // 2]
        g = g_ref[0, f].astype(F32)
        _, m_out[0, :, col], v_out[0, :, col] = adamw(g, m_ref[0, :, col], v_ref[0, :, col], g)


def unpack_d_kernel(z, w_ref, g_ref, m_ref, v_ref, w_out, m_out, v_out):
    side, rows = z.side, z.rows
    for f in range(FLOWS):
        for n in range(z.group):
            x, y = n // side, n % side
            w_out[0, pl.ds((n * FLOWS + f) * rows, rows), :] = w_ref[0, f, n if f < 2 else y * side + x]
        g = g_ref[0, f].astype(F32)
        r = pl.ds(f * rows, rows)
        _, m_out[0, r, :], v_out[0, r, :] = adamw(g, m_ref[0, r, :], v_ref[0, r, :], g)


def unpack(z, w_all, g_all, moments):
    mg, mu, md, vg, vu, vd = moments
    fb, cols, rows = z.fb, z.cols, z.rows
    last = z.layers - 1

    def unit_gu(layer, j):
        return (last - layer) * z.per_layer + j

    def unit_d(layer, i):
        return (last - layer) * z.per_layer + z.gu_units + i

    def specs(unit):
        return [
            pl.BlockSpec((1, FLOWS, z.group, rows, cols), lambda n, j: (unit(n, j), 0, 0, 0, 0)),
            pl.BlockSpec((1, FLOWS, rows, cols), lambda n, j: (unit(n, j), 0, 0, 0)),
        ]

    def column(height, width):
        return pl.BlockSpec((1, height, width), lambda n, j: (n, 0, j))

    params = pltpu.CompilerParams(vmem_limit_bytes=VMEM_LIMIT)
    part = column(rows, fb)
    like = lambda t: jax.ShapeDtypeStruct(t.shape, t.dtype)
    gate = jax.ShapeDtypeStruct((z.layers, z.d, z.ff), BF16)
    down = jax.ShapeDtypeStruct((z.layers, z.ff, z.d), BF16)
    wg, wu, mg, mu, vg, vu = pl.pallas_call(
        functools.partial(unpack_gu_kernel, z),
        grid=(z.layers, z.gu_units),
        in_specs=[*specs(unit_gu), part, part, part, part],
        out_specs=(column(z.d, fb), column(z.d, fb), part, part, part, part),
        out_shape=(gate, gate, like(mg), like(mu), like(vg), like(vu)),
        name="unpack_gu",
        compiler_params=params,
    )(w_all, g_all, mg, mu, vg, vu)
    part = column(FLOWS * rows, cols)
    wd, md, vd = pl.pallas_call(
        functools.partial(unpack_d_kernel, z),
        grid=(z.layers, z.d_units),
        in_specs=[*specs(unit_d), part, part],
        out_specs=(column(z.ff, cols), part, part),
        out_shape=(down, like(md), like(vd)),
        name="unpack_d",
        compiler_params=params,
    )(w_all, g_all, md, vd)
    return wg, wu, wd, mg, mu, md, vg, vu, vd


def normed(h):
    wide = h.astype(F32)
    return (wide * scale_of(wide)).astype(BF16)


def solution(mesh):
    group = mesh.shape["dp"]

    def device_step(x, dy, wg, wu, wd, *moments):
        x, dy = x[0], dy[0]
        z = Sizes(x.shape[0], x.shape[1], wg.shape[2], wg.shape[0], group)
        a0 = normed(x)
        p = (jax.nn.silu(mm(a0, wg[0])) * mm(a0, wu[0])).astype(BF16)
        h1 = x + mm(p, wd[0]).astype(BF16)
        a1 = normed(h1)
        w_all, g_all, _, _ = train_kernel_call(z, h1, a1, a0, dy, (wg, wu, wd), moments)
        return unpack(z, w_all, g_all, moments)

    seq, own, part, out = P(("rep", "dp")), P(), P(None, "dp"), P("rep")
    return jax.shard_map(
        device_step,
        mesh=mesh,
        in_specs=(seq, seq, own, own, own, *([part] * 6)),
        out_specs=(out, out, out, *([P("rep", "dp")] * 6)),
        check_vma=False,
    )
```

```python
import functools
import math

import jax
import jax.numpy as jnp
from jax import lax
from jax.experimental import pallas as pl
from jax.experimental.pallas import tpu as pltpu
from jax.sharding import PartitionSpec as P

F32, BF16 = jnp.float32, jnp.bfloat16
MESH = pl.DeviceIdType.MESH
VMEM_LIMIT = 64 * 1024 * 1024 - 128 * 1024
FLOWS = 4
HOPS = 3
UNPACK = 4
SLOTS = 4
HALVES = 2


def mm(a, b, dims=((1,), (0,))):
    return lax.dot_general(a, b, (dims, ((), ())), preferred_element_type=F32)


def scale_of(wide):
    return lax.rsqrt(jnp.mean(wide**2, -1, keepdims=True) + 1e-6)


def adamw(w, m, v, g):
    m = 0.9 * m + 0.1 * g
    v = 0.95 * v + 0.05 * g * g
    step = m * lax.rsqrt(v + 1e-8) + 0.1 * w
    return (w - 0.02 * step).astype(BF16), m, v


class Sizes:
    def __init__(self, tokens, d, ff, layers, group):
        self.tokens, self.d, self.ff, self.layers, self.group = tokens, d, ff, layers, group
        self.side = math.isqrt(group)
        self.rows = d // group
        self.quarters = ff // group // self.rows
        assert self.quarters == FLOWS and self.side == HOPS + 1
        self.cols = d // 8
        self.fb = 2 * self.cols
        self.gu_units = ff // self.fb
        self.d_units = d // self.cols
        self.per_layer = self.gu_units + self.d_units
        self.units = layers * self.per_layer
        self.gu_steps = self.gu_units // UNPACK
        self.pieces = ff // d
        assert layers == 2 and ff == 2 * tokens and tokens == 2 * d and self.fb * self.pieces == d


def step_kernel(
    z,
    x_in, dy_in, wg_in, wu_in, wd_in, mg_in, mu_in, md_in, vg_in, vu_in, vd_in,
    w_out, g_out, dgu_hbm, a0_hbm,
    a, at, d, hb, da, big, wgu, wd, dgu, grads,
    hrecv, hsend, hsum, lrecv, lsend, w_new, g_own, w_old, m_old, v_old,
    hs, hr, ls, lr, als, alr, ahs, ahr, own_sem, g_sem, adam_sem, w_sem, in_sem, dgu_sem, f_sem,
):
    side, rows, cols, fb = z.side, z.rows, z.cols, z.fb
    rep, me = lax.axis_index("rep"), lax.axis_index("dp")
    cx, cy = me // side, me % side
    first = [cx, cx, cy, cy]
    second = [cy, cy, cx, cx]
    way = [1, -1, 1, -1]

    def device(x, y):
        return (rep, ((x + side) % side) * side + (y + side) % side)

    def next_on_first(f):
        return device(cx + way[f], cy) if f < 2 else device(cx, cy + way[f])

    def next_on_second(f):
        return device(cx, cy + way[f]) if f < 2 else device(cx + way[f], cy)

    def behind(at_, f, n):
        return (at_ - way[f] * n + 2 * side) % side

    def remote(src, dst, send, recv, target):
        return pltpu.make_async_remote_copy(src, dst, send, recv, device_id=target, device_id_type=MESH)

    def h_copy(u, s, f):
        par = u % 2
        src = grads.at[u % SLOTS, f, pl.ds(side * behind(first[f], f, 1), side)] if s == 0 else hsend.at[par, s - 1, f]
        return remote(src, hrecv.at[par, s, f], hs.at[par, s, f], hr.at[par, s, f], next_on_first(f))

    def l_copy(u, s, f):
        par = u % 2
        return remote(lsend.at[par, s, f], lrecv.at[par, s, f], ls.at[par, s, f], lr.at[par, s, f], next_on_second(f))

    def al_copy(u, s, f):
        par = u % 2
        place = side * first[f] + behind(second[f], f, s)
        dst = w_out.at[u, f, place]
        src = w_new.at[par, f] if s == 0 else dst
        return remote(src, dst, als.at[par, s, f], alr.at[par, s, f], next_on_second(f))

    def ah_copy(u, s, f):
        par = u % 2
        dst = w_out.at[u, f, pl.ds(side * behind(first[f], f, s), side)]
        return remote(dst, dst, ahs.at[par, s, f], ahr.at[par, s, f], next_on_first(f))

    def own_copy(u, f):
        return pltpu.make_async_copy(w_new.at[u % 2, f], w_out.at[u, f, side * first[f] + second[f]], own_sem.at[u % 2, f])

    def g_copy(u):
        return pltpu.make_async_copy(g_own.at[u % 2], g_out.at[u], g_sem.at[u % 2])

    def place_of(u):
        return z.layers - 1 - u // z.per_layer, u % z.per_layer

    def adam_loads(u, start):
        layer, k = place_of(u) if start else (0, 0)

        def go(copies):
            for c in copies:
                c.start()

        def copies_gu():
            c0 = pl.multiple_of(k * fb, fb)
            r0 = pl.multiple_of(me * rows, rows)
            out = []
            for f in range(FLOWS):
                col = pl.ds(c0 + (f % 2) * cols, cols)
                w_, m_, v_ = ((wg_in, mg_in, vg_in), (wu_in, mu_in, vu_in))[f // 2]
                out.append(pltpu.make_async_copy(w_.at[layer, pl.ds(r0, rows), col], w_old.at[f], adam_sem.at[0, f]))
                out.append(pltpu.make_async_copy(m_.at[layer, :, col], m_old.at[f], adam_sem.at[1, f]))
                out.append(pltpu.make_async_copy(v_.at[layer, :, col], v_old.at[f], adam_sem.at[2, f]))
            return out

        def copies_d():
            col = pl.ds(pl.multiple_of((k - z.gu_units) * cols, cols), cols)
            out = []
            for f in range(FLOWS):
                r0 = pl.multiple_of((me * FLOWS + f) * rows, rows)
                out.append(pltpu.make_async_copy(wd_in.at[layer, pl.ds(r0, rows), col], w_old.at[f], adam_sem.at[0, f]))
                out.append(pltpu.make_async_copy(md_in.at[layer, pl.ds(f * rows, rows), col], m_old.at[f], adam_sem.at[1, f]))
                out.append(pltpu.make_async_copy(vd_in.at[layer, pl.ds(f * rows, rows), col], v_old.at[f], adam_sem.at[2, f]))
            return out

        if start:
            pl.when(k < z.gu_units)(lambda: go(copies_gu()))
            pl.when(k >= z.gu_units)(lambda: go(copies_d()))
        else:
            for c in copies_gu():
                c.wait()

    def both(x, y):
        return x.astype(F32) + y.astype(F32)

    def h_hop(u, s):
        par, slot = u % 2, u % SLOTS
        if s:
            for f in range(FLOWS):
                h_copy(u, s - 1, f).wait_recv()
                mine = grads[slot, f, pl.ds(side * behind(first[f], f, s + 1), side)]
                hsend[par, s - 1, f] = both(hrecv[par, s - 1, f], mine).astype(BF16)
        for f in range(FLOWS):
            h_copy(u, s, f).start()
            if s == HOPS - 1:
                h_copy(u, 0, f).wait_send()

    def h_end_l_start(u):
        par, slot = u % 2, u % SLOTS
        for f in range(FLOWS):
            h_copy(u, HOPS - 1, f).wait_recv()
            hsum[par, f] = both(hrecv[par, HOPS - 1, f], grads[slot, f, pl.ds(side * first[f], side)])
            lsend[par, 0, f] = hsum[par, f, behind(second[f], f, 1)].astype(BF16)
        for f in range(FLOWS):
            l_copy(u, 0, f).start()
        for f in range(FLOWS):
            for s in range(1, HOPS):
                h_copy(u, s, f).wait_send()

    def l_hop(u, s):
        par = u % 2
        for f in range(FLOWS):
            l_copy(u, s - 1, f).wait_recv()
            lsend[par, s, f] = both(lrecv[par, s - 1, f], hsum[par, f, behind(second[f], f, s + 1)]).astype(BF16)
        for f in range(FLOWS):
            l_copy(u, s, f).start()

    def l_end_al_start(u):
        par = u % 2
        adam_loads(u, False)
        for f in range(FLOWS):
            l_copy(u, HOPS - 1, f).wait_recv()
            g = both(lrecv[par, HOPS - 1, f], hsum[par, f, second[f]]).astype(BF16)
            g_own[par, f] = g
            w_new[par, f] = adamw(w_old[f].astype(F32), m_old[f], v_old[f], g.astype(F32))[0]
        for f in range(FLOWS):
            al_copy(u, 0, f).start()
            own_copy(u, f).start()
        g_copy(u).start()
        for f in range(FLOWS):
            for s in range(HOPS):
                l_copy(u, s, f).wait_send()

    def al_hop(u, s):
        for f in range(FLOWS):
            al_copy(u, s - 1, f).wait_recv()
            al_copy(u, s, f).start()

    def al_end_ah_start(u):
        for f in range(FLOWS):
            al_copy(u, HOPS - 1, f).wait_recv()
            own_copy(u, f).wait()
            ah_copy(u, 0, f).start()
        for f in range(FLOWS):
            for s in range(HOPS):
                al_copy(u, s, f).wait_send()
        g_copy(u).wait()

    def ah_hop(u, s):
        for f in range(FLOWS):
            ah_copy(u, s - 1, f).wait_recv()
            ah_copy(u, s, f).start()

    def ah_end(u):
        for f in range(FLOWS):
            ah_copy(u, HOPS - 1, f).wait_recv()
            for s in range(HOPS):
                ah_copy(u, s, f).wait_send()

    def if_unit(u, step):
        pl.when((u >= 0) & (u < z.units))(lambda: step(u))

    def slot_0(h):
        if_unit(h, lambda u: h_hop(u, 0))
        if_unit(h - 8, ah_end)
        if_unit(h - 6, al_end_ah_start)
        if_unit(h - 4, l_end_al_start)
        if_unit(h - 2, h_end_l_start)

    def slot_1(h):
        if_unit(h - 1, lambda u: h_hop(u, 2))
        if_unit(h - 3, lambda u: l_hop(u, 2))
        if_unit(h - 5, lambda u: al_hop(u, 2))
        if_unit(h - 7, lambda u: ah_hop(u, 2))
        if_unit(h - 3, lambda u: adam_loads(u, True))

    def slot_2(h):
        if_unit(h, lambda u: h_hop(u, 1))
        if_unit(h - 2, lambda u: l_hop(u, 1))
        if_unit(h - 4, lambda u: al_hop(u, 1))
        if_unit(h - 6, lambda u: ah_hop(u, 1))

    tile = z.tokens // HALVES
    last = z.layers - 1
    n_gu, n_d = z.gu_units, z.d_units
    a_end = n_gu - 1
    c_end = a_end + n_d
    a2_end = c_end + n_gu
    c2_end = a2_end + n_d
    wide_tile = z.tokens // 8

    def rows_of(t, size):
        return pl.ds(pl.multiple_of(t * size, size), size)

    def loop(lo, hi, body):
        lax.fori_loop(lo, hi, lambda i, c: (body(i), c)[1], 0)

    def weight_loads(layer, j, with_down):
        buf, cols_j = j % 2, rows_of(j, fb)
        out = [
            pltpu.make_async_copy(wg_in.at[layer, :, cols_j], wgu.at[buf, :, pl.ds(0, fb)], w_sem.at[buf, 0]),
            pltpu.make_async_copy(wu_in.at[layer, :, cols_j], wgu.at[buf, :, pl.ds(fb, fb)], w_sem.at[buf, 1]),
        ]
        if with_down:
            out.append(pltpu.make_async_copy(wd_in.at[layer, cols_j, :], wd.at[buf], w_sem.at[buf, 2]))
        return out

    def dgu_load(j):
        return pltpu.make_async_copy(dgu_hbm.at[j], dgu.at[j % 2], dgu_sem.at[j % 2])

    def dgu_store(j):
        return pltpu.make_async_copy(dgu.at[j % 2], dgu_hbm.at[j], dgu_sem.at[j % 2])

    def start(copies):
        for c in copies:
            c.start()

    def wait(copies):
        for c in copies:
            c.wait()

    def normed_of(wide):
        return (wide * scale_of(wide)).astype(BF16)

    def f1_block(j):
        wait(weight_loads(0, j, False))
        gu = mm(a[...], wgu[j % 2])
        gate, up = gu[:, :fb], gu[:, fb:]
        c0 = j * fb
        big[rows_of(c0 // z.tokens, z.tokens), pl.ds(pl.multiple_of(c0 % z.tokens, fb), fb)] = (jax.nn.silu(gate) * up).astype(BF16)
        pl.when(j + 2 < n_gu)(lambda: start(weight_loads(0, j + 2, False)))
        pl.when(j + 2 >= n_gu)(lambda: start(weight_loads(last, j + 2 - n_gu, True)))

    def f2_loads(n):
        buf = n % 2
        out = []
        for k in range(z.pieces):
            dst = at.at[:, pl.ds(pl.multiple_of(buf * d_half + k * fb, fb), fb)]
            out.append(pltpu.make_async_copy(wd_in.at[0, pl.ds(k * z.d, z.d), rows_of(n, fb)], dst, f_sem.at[buf, k]))
        return out

    d_half = z.tokens // 2

    def f2_block(n):
        wait(f2_loads(n))

        def part(t):
            acc = None
            for k in range(z.pieces):
                r = pl.ds(pl.multiple_of((k // 2) * z.tokens + t * tile, tile), tile)
                w_k = at[:, pl.ds(pl.multiple_of((n % 2) * d_half + k * fb, fb), fb)]
                one = mm(big[r, pl.ds((k % 2) * z.d, z.d)], w_k)
                acc = one if acc is None else acc + one
            here = (rows_of(t, tile), rows_of(n, fb))
            hb[here] = both(hb[here], acc.astype(BF16)).astype(BF16)

        loop(0, HALVES, part)
        pl.when(n + 2 < z.d // fb)(lambda: start(f2_loads(n + 2)))

    def first_norm(t):
        r = rows_of(t, wide_tile)
        a[r, :] = normed_of(hb[r, :].astype(F32))

    def norm_and_transpose(t):
        r = rows_of(t, wide_tile)
        new = normed_of(hb[r, :].astype(F32))
        a[r, :] = new
        at[:, r] = new.T

    def transpose_tile(t):
        r = rows_of(t, wide_tile)
        at[:, r] = a[r, :].T

    def backward_tile(t, j):
        buf, r = j % 2, rows_of(t, tile)
        gu = mm(a[r, :], wgu[buf])
        gate, up = gu[:, :fb], gu[:, fb:]
        dp = mm(d[r, :], wd[buf], ((1,), (1,))).astype(BF16).astype(F32)
        sig = jax.nn.sigmoid(gate)
        silu = gate * sig
        big[rows_of(j, fb), r] = (silu * up).astype(BF16).T
        dgu[buf, r, pl.ds(fb, fb)] = (dp * silu).astype(BF16)
        dgu[buf, r, pl.ds(0, fb)] = (dp * up * (sig * (1 + gate * (1 - sig)))).astype(BF16)

    def store_block(slot, f, dev, value):
        x, y = dev // side, dev % side
        grads[slot, f, x * side + y if f < 2 else y * side + x] = value

    def gu_grads(layer, j, u):
        pl.when(layer == last)(lambda: dgu_store(j).start())
        out = mm(at[...], dgu[j % 2]).astype(BF16)
        for dev in range(z.group):
            for f in range(FLOWS):
                store_block(u % SLOTS, f, dev, out[dev * rows : (dev + 1) * rows, f * cols : (f + 1) * cols])

        @pl.when(layer == last)
        def _():
            dgu_store(j).wait()

            @pl.when(j + 2 < n_gu)
            def _():
                start(weight_loads(last, j + 2, True))

            @pl.when(j + 2 >= n_gu)
            def _():
                start(weight_loads(last, j + 2 - n_gu, False))
                dgu_load(j + 2 - n_gu).start()

        pl.when((layer != last) & (j + 2 < n_gu))(lambda: start(weight_loads(0, j + 2, True)))

    def d_grads(t, pair, u):
        devices = z.group // z.pieces
        out = mm(big[rows_of(t, z.d), :], d[:, rows_of(pair, 2 * cols)]).astype(BF16)
        for n in range(devices):
            for f in range(FLOWS):
                r0 = (n * FLOWS + f) * rows
                for k in range(2):
                    store_block((u + k) % SLOTS, f, t * devices + n, out[r0 : r0 + rows, k * cols : (k + 1) * cols])

    def da_block(k):
        buf = k % 2
        wait(weight_loads(last, k, False))
        dgu_load(k).wait()

        def part(t, first):
            r = rows_of(t, tile)
            new = mm(dgu[buf, r, :], wgu[buf], ((1,), (1,)))
            da[r, :] = new if first else da[r, :] + new

        pl.when(k == 0)(lambda: loop(0, HALVES, lambda t: part(t, True)))
        pl.when(k != 0)(lambda: loop(0, HALVES, lambda t: part(t, False)))

        @pl.when(k + 2 < n_gu)
        def _():
            start(weight_loads(last, k + 2, False))
            dgu_load(k + 2).start()

        pl.when(k + 2 >= n_gu)(lambda: start(weight_loads(0, k + 2 - n_gu, True)))

    def norm_backward(t):
        r = rows_of(t, wide_tile)
        wide = hb[r, :].astype(F32)
        scale = scale_of(wide)
        by_a = da[r, :].astype(BF16).astype(F32)
        inner = jnp.mean(by_a * wide, -1, keepdims=True)
        d[r, :] = both(d[r, :], (scale * by_a - wide * (scale**3 * inner)).astype(BF16)).astype(BF16)

    def a0_load():
        return pltpu.make_async_copy(a0_hbm, a, in_sem.at[0])

    per_pair = 2 * n_gu // n_d

    def piece(h, n):
        is_gu = (h < a_end) | ((h >= c_end) & (h < a2_end))
        layer, j = jnp.where(h < a_end, last, 0), jnp.where(h < a_end, h + 1, h - c_end)
        i = jnp.where(h < c_end, h - a_end, h - a2_end)
        is_d = ((h >= a_end) & (h < c_end)) | ((h >= a2_end) & (h < c2_end))
        is_da = (h >= a_end) & (h < c_end)

        if n == 0:

            @pl.when(h == c_end)
            def _():
                a0_load().wait()
                loop(0, 8, transpose_tile)

            pl.when(h == a_end)(lambda: a0_load().start())

        @pl.when(is_gu)
        def _():
            if n == 0:
                wait(weight_loads(layer, j, True))
            if n < HALVES:
                backward_tile(n, j)
            else:
                gu_grads(layer, j, h + 1)

        @pl.when(is_d & (i % 2 == 0))
        def _():
            if n < 2:
                half = z.pieces // 2
                loop(n * half, (n + 1) * half, lambda t: d_grads(t, i // 2, h + 1))

        @pl.when(is_da & (i % 2 == 1))
        def _():
            da_block((i // 2) * per_pair + 1 + n)

        if n == 2:

            @pl.when(is_da & (i % 2 == 0))
            def _():
                da_block((i // 2) * per_pair)

            @pl.when(h == c_end - 1)
            def _():
                loop(0, 8, norm_backward)

    barrier = pltpu.get_barrier_semaphore()
    for f in range(FLOWS):
        pl.semaphore_signal(barrier, inc=1, device_id=next_on_first(f), device_id_type=MESH)
    half = pl.ds(0, z.tokens // 2), pl.ds(z.tokens // 2, z.tokens // 2)
    x_loads = [pltpu.make_async_copy(x_in.at[half[n]], hb.at[half[n]], in_sem.at[n]) for n in range(2)]
    dy_load = pltpu.make_async_copy(dy_in, d, in_sem.at[0])
    a0_store = pltpu.make_async_copy(a, a0_hbm, in_sem.at[1])
    start(x_loads + weight_loads(0, 0, False))
    for n in range(2):
        x_loads[n].wait()
        loop(4 * n, 4 * n + 4, first_norm)
    a0_store.start()
    dy_load.start()
    start(weight_loads(0, 1, False) + f2_loads(0) + f2_loads(1))
    loop(0, n_gu, f1_block)
    loop(0, z.d // fb, f2_block)
    a0_store.wait()
    loop(0, 8, norm_and_transpose)
    dy_load.wait()
    wait(weight_loads(last, 0, True))
    loop(0, HALVES, lambda t: backward_tile(t, 0))
    gu_grads(last, 0, 0)
    pl.semaphore_wait(barrier, FLOWS)

    def half_step(h):
        slot_0(h)
        piece(h, 0)
        slot_1(h)
        piece(h, 1)
        slot_2(h)
        piece(h, 2)

    loop(0, z.units + 8, half_step)


def train_kernel_call(z, x, dy, weights, moments):
    side, rows, cols, fb = z.side, z.rows, z.cols, z.fb
    dma = pltpu.SemaphoreType.DMA
    hbm = pl.BlockSpec(memory_space=pl.ANY)
    out_shape = (
        jax.ShapeDtypeStruct((z.units, FLOWS, z.group, rows, cols), BF16),
        jax.ShapeDtypeStruct((z.units, FLOWS, rows, cols), BF16),
        jax.ShapeDtypeStruct((z.gu_units, z.tokens, 2 * fb), BF16),
        jax.ShapeDtypeStruct((z.tokens, z.d), BF16),
    )
    scratch = [
        pltpu.VMEM((z.tokens, z.d), BF16),
        pltpu.VMEM((z.d, z.tokens), BF16),
        pltpu.VMEM((z.tokens, z.d), BF16),
        pltpu.VMEM((z.tokens, z.d), BF16),
        pltpu.VMEM((z.tokens, z.d), F32),
        pltpu.VMEM((z.ff, z.tokens), BF16),
        pltpu.VMEM((2, z.d, 2 * fb), BF16),
        pltpu.VMEM((2, fb, z.d), BF16),
        pltpu.VMEM((2, z.tokens, 2 * fb), BF16),
        pltpu.VMEM((SLOTS, FLOWS, z.group, rows, cols), BF16),
        pltpu.VMEM((2, HOPS, FLOWS, side, rows, cols), BF16),
        pltpu.VMEM((2, HOPS - 1, FLOWS, side, rows, cols), BF16),
        pltpu.VMEM((2, FLOWS, side, rows, cols), F32),
        pltpu.VMEM((2, HOPS, FLOWS, rows, cols), BF16),
        pltpu.VMEM((2, HOPS, FLOWS, rows, cols), BF16),
        pltpu.VMEM((2, FLOWS, rows, cols), BF16),
        pltpu.VMEM((2, FLOWS, rows, cols), BF16),
        pltpu.VMEM((FLOWS, rows, cols), BF16),
        pltpu.VMEM((FLOWS, rows, cols), F32),
        pltpu.VMEM((FLOWS, rows, cols), F32),
        *[dma((2, HOPS, FLOWS)) for _ in range(8)],
        dma((2, FLOWS)),
        dma((2,)),
        dma((3, FLOWS)),
        dma((2, 3)),
        dma((2,)),
        dma((2,)),
        dma((2, z.pieces)),
    ]
    return pl.pallas_call(
        functools.partial(step_kernel, z),
        out_shape=out_shape,
        in_specs=[hbm] * 11,
        out_specs=(hbm,) * 4,
        scratch_shapes=scratch,
        name="train_step",
        compiler_params=pltpu.CompilerParams(collective_id=0, has_side_effects=True, vmem_limit_bytes=VMEM_LIMIT),
    )(x, dy, *weights, *moments)


def unpack_kernel(z, w_ref, g_ref, *refs):
    side, rows, cols = z.side, z.rows, z.cols
    mg, mu, md, vg, vu, vd, wg_out, wu_out, wd_out, *new = refs
    mg_new, mu_new, md_new, vg_new, vu_new, vd_new = new

    def step(f, k, m, v, m_new, v_new, place):
        g = g_ref[k, f].astype(F32)
        _, m_new[place], v_new[place] = adamw(g, m[place], v[place], g)

    @pl.when(pl.program_id(1) < z.gu_steps)
    def _():
        for k in range(UNPACK):
            for f in range(FLOWS):
                col = pl.ds((2 * k + f % 2) * cols, cols)
                for dev in range(z.group):
                    place = dev if f < 2 else dev % side * side + dev // side
                    (wg_out, wu_out)[f // 2][0, pl.ds(dev * rows, rows), col] = w_ref[k, f, place]
                moments = ((mg, vg, mg_new, vg_new), (mu, vu, mu_new, vu_new))[f // 2]
                step(f, k, *moments, (0, slice(None), col))

    @pl.when(pl.program_id(1) >= z.gu_steps)
    def _():
        for k in range(UNPACK):
            col = pl.ds(k * cols, cols)
            for f in range(FLOWS):
                for dev in range(z.group):
                    place = dev if f < 2 else dev % side * side + dev // side
                    wd_out[0, pl.ds((dev * FLOWS + f) * rows, rows), col] = w_ref[k, f, place]
                step(f, k, md, vd, md_new, vd_new, (0, pl.ds(f * rows, rows), col))


def unpack(z, w_all, g_all, moments):
    cols, rows = z.cols, z.rows
    steps = z.per_layer // UNPACK

    def unit(n, j):
        return (z.layers - 1 - n) * steps + j

    def gu(height):
        return pl.BlockSpec((1, height, 2 * UNPACK * cols), lambda n, j: (n, 0, jnp.minimum(j, z.gu_steps - 1)))

    def down(height):
        return pl.BlockSpec((1, height, UNPACK * cols), lambda n, j: (n, 0, jnp.maximum(j - z.gu_steps, 0)))

    specs = [gu(rows), gu(rows), down(FLOWS * rows)] * 2
    like = [jax.ShapeDtypeStruct(t.shape, t.dtype) for t in moments]
    gate = jax.ShapeDtypeStruct((z.layers, z.d, z.ff), BF16)
    return pl.pallas_call(
        functools.partial(unpack_kernel, z),
        grid=(z.layers, steps),
        in_specs=[
            pl.BlockSpec((UNPACK, FLOWS, z.group, rows, cols), lambda n, j: (unit(n, j), 0, 0, 0, 0)),
            pl.BlockSpec((UNPACK, FLOWS, rows, cols), lambda n, j: (unit(n, j), 0, 0, 0)),
            *specs,
        ],
        out_specs=(gu(z.d), gu(z.d), down(z.ff), *specs),
        out_shape=(gate, gate, jax.ShapeDtypeStruct((z.layers, z.ff, z.d), BF16), *like),
        name="unpack",
        compiler_params=pltpu.CompilerParams(vmem_limit_bytes=VMEM_LIMIT),
    )(w_all, g_all, *moments)


def solution(mesh):
    group = mesh.shape["dp"]

    def device_step(x, dy, wg, wu, wd, *moments):
        x, dy = x[0], dy[0]
        z = Sizes(x.shape[0], x.shape[1], wg.shape[2], wg.shape[0], group)
        w_all, g_all, *_ = train_kernel_call(z, x, dy, (wg, wu, wd), moments)
        return unpack(z, w_all, g_all, moments)

    seq, own, part, out = P(("rep", "dp")), P(), P(None, "dp"), P("rep")
    return jax.shard_map(
        device_step,
        mesh=mesh,
        in_specs=(seq, seq, own, own, own, *([part] * 6)),
        out_specs=(out, out, out, *([P("rep", "dp")] * 6)),
        check_vma=False,
    )
```

```python
import functools
import math

import jax
import jax.numpy as jnp
from jax import lax
from jax.experimental import pallas as pl
from jax.experimental.pallas import tpu as pltpu
from jax.sharding import PartitionSpec as P

F32, BF16 = jnp.float32, jnp.bfloat16
MESH = pl.DeviceIdType.MESH
VMEM_LIMIT = 64 * 1024 * 1024 - 128 * 1024
FLOWS = 4
COPIES = 3
UNPACK = 4
LAST = 2
HURRIED = 2
SETS = 4
AH_SETS = 8
SLOTS = 4
HALVES = 2


def mm(a, b, dims=((1,), (0,))):
    return lax.dot_general(a, b, (dims, ((), ())), preferred_element_type=F32)


def scale_of(wide):
    return lax.rsqrt(jnp.mean(wide**2, -1, keepdims=True) + 1e-6)


def adamw(w, m, v, g):
    m = 0.9 * m + 0.1 * g
    v = 0.95 * v + 0.05 * g * g
    step = m * lax.rsqrt(v + 1e-8) + 0.1 * w
    return (w - 0.02 * step).astype(BF16), m, v


class Sizes:
    def __init__(self, tokens, d, ff, layers, group):
        self.tokens, self.d, self.ff, self.layers, self.group = tokens, d, ff, layers, group
        self.side = math.isqrt(group)
        self.rows = d // group
        self.quarters = ff // group // self.rows
        assert self.quarters == FLOWS and self.side == 4
        self.cols = d // 8
        self.fb = 2 * self.cols
        self.gu_units = ff // self.fb
        self.d_units = d // self.cols
        self.per_layer = self.gu_units + self.d_units
        self.units = layers * self.per_layer
        self.gu_steps = self.gu_units // UNPACK
        self.pieces = ff // d
        assert layers == 2 and ff == 2 * tokens and tokens == 2 * d and self.fb * self.pieces == d


def step_kernel(
    z,
    x_in, dy_in, wg_in, wu_in, wd_in, mg_in, mu_in, md_in, vg_in, vu_in, vd_in,
    w_out, g_out, dgu_hbm, a0_hbm,
    a, at, d, hb, da, big, wgu, wd, dgu, grads,
    hrecv, hsend, hsum, lrecv, lsend, w_new, g_own, w_old, m_old, v_old, lx,
    hs, hr, ls, lr, als, alr, ahs, ahr, own_sem, g_sem, adam_sem, w_sem, in_sem, dgu_sem, f_sem, x_sem,
):
    side, rows, cols, fb = z.side, z.rows, z.cols, z.fb
    rep, me = lax.axis_index("rep"), lax.axis_index("dp")
    cx, cy = me // side, me % side
    first = [cx, cx, cy, cy]
    second = [cy, cy, cx, cx]
    way = [1, -1, 1, -1]

    def device(x, y):
        return (rep, ((x + side) % side) * side + (y + side) % side)

    def on_first(f, s):
        n = way[f] * (-1 if s == 1 else 1)
        return device(cx + n, cy) if f < 2 else device(cx, cy + n)

    def on_second(f, s, far=1):
        n = way[f] * (-1 if s == 1 else far)
        return device(cx, cy + n) if f < 2 else device(cx + n, cy)

    def behind(at_, f, n):
        return (at_ - way[f] * n + 2 * side) % side

    def remote(src, dst, send, recv, target):
        return pltpu.make_async_remote_copy(src, dst, send, recv, device_id=target, device_id_type=MESH)

    def h_copy(u, s, f):
        par = u % 2
        src = hsend.at[par, f] if s == 2 else grads.at[u % SLOTS, f, pl.ds(side * behind(first[f], f, 2 - s), side)]
        return remote(src, hrecv.at[par, s, f], hs.at[par], hr.at[par, (s + 1) // 2], on_first(f, s))

    def l_copy(u, s, f):
        par = u % 2
        return remote(lsend.at[par, s, f], lrecv.at[par, s, f], ls.at[par], lr.at[par, (s + 1) // 2], on_second(f, s))

    def al_copy(u, s, f):
        k = u % SETS
        dst = w_out.at[u, f, side * first[f] + behind(second[f], f, s // 2)]
        return remote(w_new.at[u % 2, f] if s < 2 else dst, dst, als.at[k], alr.at[k, (s + 1) // 2], on_second(f, s))

    def ah_copy(u, s, f):
        k = u % AH_SETS
        dst = w_out.at[u, f, pl.ds(side * behind(first[f], f, s // 2), side)]
        return remote(dst, dst, ahs.at[k], ahr.at[k, (s + 1) // 2], on_first(f, s))

    def own_copy(u, f):
        return pltpu.make_async_copy(w_new.at[u % 2, f], w_out.at[u, f, side * first[f] + second[f]], own_sem.at[u % 2])

    def wait_for(copies, big, sem):
        size = (hrecv if big else lrecv).at[0, pl.ds(0, copies)]
        pltpu.make_async_copy(size, size, sem).wait()

    def g_copy(u):
        return pltpu.make_async_copy(g_own.at[u % 2], g_out.at[u], g_sem.at[u % 2])

    def place_of(u):
        return z.layers - 1 - u // z.per_layer, u % z.per_layer

    def adam_loads(u, start):
        layer, k = place_of(u)
        par = u % 2

        def go(copies):
            for c in copies:
                c.start()

        def copies_gu():
            c0 = pl.multiple_of(k * fb, fb)
            r0 = pl.multiple_of(me * rows, rows)
            out = []
            for f in range(FLOWS):
                col = pl.ds(c0 + (f % 2) * cols, cols)
                w_, m_, v_ = ((wg_in, mg_in, vg_in), (wu_in, mu_in, vu_in))[f // 2]
                out.append(pltpu.make_async_copy(w_.at[layer, pl.ds(r0, rows), col], w_old.at[par, f], adam_sem.at[par, 0]))
                out.append(pltpu.make_async_copy(m_.at[layer, :, col], m_old.at[par, f], adam_sem.at[par, 1]))
                out.append(pltpu.make_async_copy(v_.at[layer, :, col], v_old.at[par, f], adam_sem.at[par, 2]))
            return out

        def copies_d():
            col = pl.ds(pl.multiple_of((k - z.gu_units) * cols, cols), cols)
            out = []
            for f in range(FLOWS):
                r0 = pl.multiple_of((me * FLOWS + f) * rows, rows)
                out.append(pltpu.make_async_copy(wd_in.at[layer, pl.ds(r0, rows), col], w_old.at[par, f], adam_sem.at[par, 0]))
                out.append(pltpu.make_async_copy(md_in.at[layer, pl.ds(f * rows, rows), col], m_old.at[par, f], adam_sem.at[par, 1]))
                out.append(pltpu.make_async_copy(vd_in.at[layer, pl.ds(f * rows, rows), col], v_old.at[par, f], adam_sem.at[par, 2]))
            return out

        if start:
            pl.when(k < z.gu_units)(lambda: go(copies_gu()))
            pl.when(k >= z.gu_units)(lambda: go(copies_d()))
        else:
            for n, old in enumerate((w_old, m_old, v_old)):
                pltpu.make_async_copy(old.at[par], old.at[par], adam_sem.at[par, n]).wait()

    def start(copies):
        for c in copies:
            c.start()

    def wait(copies):
        for c in copies:
            c.wait()

    def both(x, y):
        return x.astype(F32) + y.astype(F32)

    flows = range(FLOWS)

    def group(f, n):
        return pl.ds(side * behind(first[f], f, n), side)

    def h_a(u):
        for f in flows:
            start([h_copy(u, 0, f), h_copy(u, 1, f)])

    def h_b(u):
        par = u % 2
        wait_for(1, True, hr.at[par, 0])
        for f in flows:
            hsend[par, f] = both(hrecv[par, 0, f], grads[u % SLOTS, f, group(f, 3)]).astype(BF16)
        for f in flows:
            h_copy(u, 2, f).start()

    def h_end(u):
        par = u % 2
        wait_for(2, True, hr.at[par, 1])
        for f in flows:
            hsum[par, f] = both(hrecv[par, 1, f], hrecv[par, 2, f]) + grads[u % SLOTS, f, group(f, 0)].astype(F32)

    def l_a(u):
        par = u % 2
        h_end(u)
        for f in flows:
            for s in range(2):
                lsend[par, s, f] = hsum[par, f, behind(second[f], f, 2 - s)].astype(BF16)
        for f in flows:
            start([l_copy(u, 0, f), l_copy(u, 1, f)])
        wait_for(COPIES, True, hs.at[par])

    def step_weight(u, f, total):
        par, g = u % 2, total.astype(BF16)
        g_own[par, f] = g
        w_new[par, f] = adamw(w_old[par, f].astype(F32), m_old[par, f], v_old[par, f], g.astype(F32))[0]

    def l_b(u):
        par = u % 2
        wait_for(1, False, lr.at[par, 0])
        for f in flows:
            lsend[par, 2, f] = both(lrecv[par, 0, f], hsum[par, f, behind(second[f], f, 3)]).astype(BF16)
        for f in flows:
            l_copy(u, 2, f).start()

    def al_a(u):
        par = u % 2
        adam_loads(u, False)
        wait_for(2, False, lr.at[par, 1])
        for f in flows:
            step_weight(u, f, both(lrecv[par, 1, f], lrecv[par, 2, f]) + hsum[par, f, second[f]])
        for f in flows:
            start([al_copy(u, 0, f), al_copy(u, 1, f), own_copy(u, f)])
        g_copy(u).start()
        wait_for(COPIES, False, ls.at[par])

    def al_b(u):
        wait_for(1, False, alr.at[u % SETS, 0])
        for f in flows:
            al_copy(u, 2, f).start()

    def al_end(u):
        wait_for(2, False, alr.at[u % SETS, 1])
        wait_for(COPIES, False, als.at[u % SETS])
        wait_for(1, False, own_sem.at[u % 2])
        g_copy(u).wait()

    def ah_a(u):
        for f in flows:
            start([ah_copy(u, 0, f), ah_copy(u, 1, f)])

    def ah_b(u):
        wait_for(1, True, ahr.at[u % AH_SETS, 0])
        for f in flows:
            ah_copy(u, 2, f).start()

    def ah_end(u):
        wait_for(2, True, ahr.at[u % AH_SETS, 1])
        wait_for(COPIES, True, ahs.at[u % AH_SETS])

    def if_unit(u, step, lo=0, hi=z.units):
        pl.when((u >= lo) & (u < hi))(lambda: step(u))

    def l_last(u, f):
        return remote(lsend.at[u % 2, 2, f], lx.at[u % 2, f], x_sem.at[0, u % 2], x_sem.at[1, u % 2], on_second(f, 2, 2))

    def al_last(u, s, f):
        if s < 2:
            return al_copy(u, s, f)
        dst = w_out.at[u, f, side * first[f] + second[f]]
        return remote(w_new.at[u % 2, f], dst, x_sem.at[2, u % 2], x_sem.at[3, u % 2], on_second(f, 2, 2))

    def wait_for_last(u, send, recv, far):
        wait_for(1, False, recv.at[0])
        wait_for(1, False, recv.at[1])
        wait_for(1, False, x_sem.at[far + 1, u % 2])
        wait_for(2, False, send)
        wait_for(1, False, x_sem.at[far, u % 2])

    def l_a_last(u):
        h_end(u)
        par = u % 2
        for f in flows:
            for s, n in enumerate((3, 1, 2)):
                lsend[par, s, f] = hsum[par, f, behind(second[f], f, n)].astype(BF16)
        for f in flows:
            start([l_copy(u, 0, f), l_copy(u, 1, f), l_last(u, f)])
        wait_for(COPIES, True, hs.at[par])

    def al_a_last(u):
        par = u % 2
        adam_loads(u, False)
        wait_for_last(u, ls.at[par], lr.at[par], 0)
        for f in flows:
            step_weight(u, f, both(lrecv[par, 0, f], lrecv[par, 1, f]) + both(lx[par, f], hsum[par, f, second[f]]))
        for f in flows:
            start([al_last(u, s, f) for s in range(COPIES)] + [own_copy(u, f)])
        g_copy(u).start()

    def ah_a_last(u):
        wait_for_last(u, als.at[u % SETS], alr.at[u % SETS], 2)
        wait_for(1, False, own_sem.at[u % 2])
        ah_a(u)
        g_copy(u).wait()

    last_ones = z.units - LAST
    hurried = last_ones - HURRIED

    def slot_0(h):
        if_unit(h - 2, l_b, 0, last_ones)
        if_unit(h, h_a)
        if_unit(h - 4, al_end, hurried, last_ones)
        if_unit(h - 4, ah_a, hurried, last_ones)
        if_unit(h - 2, al_a_last, last_ones)
        if_unit(h - 4, ah_end, last_ones)

    def slot_1(h):
        if_unit(h - 3, al_b, 0, last_ones)
        if_unit(h - 1, l_a, 0, last_ones)
        if_unit(h - 1, l_a_last, last_ones)
        if_unit(h - 6, ah_end, 0, hurried)
        if_unit(h - 5, ah_end, hurried, last_ones)
        if_unit(h - 4, al_end, 0, hurried)
        if_unit(h - 4, ah_a, 0, hurried)
        if_unit(h - 3, ah_b, last_ones)
        if_unit(h - 1, lambda u: adam_loads(u, True))

    def slot_2(h):
        if_unit(h, h_b)
        if_unit(h - 2, al_a, 0, last_ones)
        if_unit(h - 5, ah_b, 0, hurried)
        if_unit(h - 4, ah_b, hurried, last_ones)
        if_unit(h - 2, ah_a_last, last_ones)

    tile = z.tokens // HALVES
    last = z.layers - 1
    n_gu, n_d = z.gu_units, z.d_units
    a_end = n_gu - 1
    c_end = a_end + n_d
    a2_end = c_end + n_gu
    c2_end = a2_end + n_d
    wide_tile = z.tokens // 8

    def rows_of(t, size):
        return pl.ds(pl.multiple_of(t * size, size), size)

    def loop(lo, hi, body):
        lax.fori_loop(lo, hi, lambda i, c: (body(i), c)[1], 0)

    def weight_loads(layer, j, with_down):
        buf, cols_j = j % 2, rows_of(j, fb)
        out = [
            pltpu.make_async_copy(wg_in.at[layer, :, cols_j], wgu.at[buf, :, pl.ds(0, fb)], w_sem.at[buf, 0]),
            pltpu.make_async_copy(wu_in.at[layer, :, cols_j], wgu.at[buf, :, pl.ds(fb, fb)], w_sem.at[buf, 1]),
        ]
        if with_down:
            out.append(pltpu.make_async_copy(wd_in.at[layer, cols_j, :], wd.at[buf], w_sem.at[buf, 2]))
        return out

    def dgu_load(j):
        return pltpu.make_async_copy(dgu_hbm.at[j], dgu.at[j % 2], dgu_sem.at[j % 2])

    def dgu_store(j):
        return pltpu.make_async_copy(dgu.at[j % 2], dgu_hbm.at[j], dgu_sem.at[j % 2])

    def normed_of(wide):
        return (wide * scale_of(wide)).astype(BF16)

    def f1_block(j):
        wait(weight_loads(0, j, False))
        gu = mm(a[...], wgu[j % 2])
        gate, up = gu[:, :fb], gu[:, fb:]
        c0 = j * fb
        big[rows_of(c0 // z.tokens, z.tokens), pl.ds(pl.multiple_of(c0 % z.tokens, fb), fb)] = (jax.nn.silu(gate) * up).astype(BF16)
        pl.when(j + 2 < n_gu)(lambda: start(weight_loads(0, j + 2, False)))
        pl.when(j + 2 >= n_gu)(lambda: start(weight_loads(last, j + 2 - n_gu, True)))

    def f2_loads(n):
        buf = n % 2
        out = []
        for k in range(z.pieces):
            dst = at.at[:, pl.ds(pl.multiple_of(buf * d_half + k * fb, fb), fb)]
            out.append(pltpu.make_async_copy(wd_in.at[0, pl.ds(k * z.d, z.d), rows_of(n, fb)], dst, f_sem.at[buf]))
        return out

    d_half = z.tokens // 2

    def f2_block(n):
        both_k = at.at[:, pl.ds(0, d_half)]
        pltpu.make_async_copy(both_k, both_k, f_sem.at[n % 2]).wait()

        def part(t):
            acc = None
            for k in range(z.pieces):
                r = pl.ds(pl.multiple_of((k // 2) * z.tokens + t * tile, tile), tile)
                w_k = at[:, pl.ds(pl.multiple_of((n % 2) * d_half + k * fb, fb), fb)]
                one = mm(big[r, pl.ds((k % 2) * z.d, z.d)], w_k)
                acc = one if acc is None else acc + one
            here = (rows_of(t, tile), rows_of(n, fb))
            hb[here] = both(hb[here], acc.astype(BF16)).astype(BF16)

        loop(0, HALVES, part)
        pl.when(n + 2 < z.d // fb)(lambda: start(f2_loads(n + 2)))

    def first_norm(t):
        r = rows_of(t, wide_tile)
        a[r, :] = normed_of(hb[r, :].astype(F32))

    def norm_and_transpose(t):
        r = rows_of(t, wide_tile)
        new = normed_of(hb[r, :].astype(F32))
        a[r, :] = new
        at[:, r] = new.T

    def transpose_tile(t):
        r = rows_of(t, wide_tile)
        at[:, r] = a[r, :].T

    def backward_tile(t, j):
        buf, r = j % 2, rows_of(t, tile)
        gu = mm(a[r, :], wgu[buf])
        gate, up = gu[:, :fb], gu[:, fb:]
        dp = mm(d[r, :], wd[buf], ((1,), (1,))).astype(BF16).astype(F32)
        sig = jax.nn.sigmoid(gate)
        silu = gate * sig
        big[rows_of(j, fb), r] = (silu * up).astype(BF16).T
        dgu[buf, r, pl.ds(fb, fb)] = (dp * silu).astype(BF16)
        dgu[buf, r, pl.ds(0, fb)] = (dp * up * (sig * (1 + gate * (1 - sig)))).astype(BF16)

    def store_block(slot, f, dev, value):
        x, y = dev // side, dev % side
        grads[slot, f, x * side + y if f < 2 else y * side + x] = value

    def gu_grads(layer, j, u):
        pl.when(layer == last)(lambda: dgu_store(j).start())
        out = mm(at[...], dgu[j % 2]).astype(BF16)
        for dev in range(z.group):
            for f in range(FLOWS):
                store_block(u % SLOTS, f, dev, out[dev * rows : (dev + 1) * rows, f * cols : (f + 1) * cols])

        @pl.when(layer == last)
        def _():
            dgu_store(j).wait()

            @pl.when(j + 2 < n_gu)
            def _():
                start(weight_loads(last, j + 2, True))

            @pl.when(j + 2 >= n_gu)
            def _():
                start(weight_loads(last, j + 2 - n_gu, False))
                dgu_load(j + 2 - n_gu).start()

        pl.when((layer != last) & (j + 2 < n_gu))(lambda: start(weight_loads(0, j + 2, True)))

    def d_grads(t, pair, u):
        devices = z.group // 2
        out = mm(big[rows_of(t, z.ff // 2), :], d[:, rows_of(pair, 2 * cols)]).astype(BF16)
        for n in range(devices):
            for f in range(FLOWS):
                r0 = (n * FLOWS + f) * rows
                for k in range(2):
                    store_block((u + k) % SLOTS, f, t * devices + n, out[r0 : r0 + rows, k * cols : (k + 1) * cols])

    def da_block(k):
        buf = k % 2
        wait(weight_loads(last, k, False))
        dgu_load(k).wait()

        def part(t, first):
            r = rows_of(t, tile)
            new = mm(dgu[buf, r, :], wgu[buf], ((1,), (1,)))
            da[r, :] = new if first else da[r, :] + new

        pl.when(k == 0)(lambda: loop(0, HALVES, lambda t: part(t, True)))
        pl.when(k != 0)(lambda: loop(0, HALVES, lambda t: part(t, False)))

        @pl.when(k + 2 < n_gu)
        def _():
            start(weight_loads(last, k + 2, False))
            dgu_load(k + 2).start()

        pl.when(k + 2 >= n_gu)(lambda: start(weight_loads(0, k + 2 - n_gu, True)))

    def norm_backward(t):
        r = rows_of(t, wide_tile)
        wide = hb[r, :].astype(F32)
        scale = scale_of(wide)
        by_a = da[r, :].astype(BF16).astype(F32)
        inner = jnp.mean(by_a * wide, -1, keepdims=True)
        d[r, :] = both(d[r, :], (scale * by_a - wide * (scale**3 * inner)).astype(BF16)).astype(BF16)

    def a0_load():
        return pltpu.make_async_copy(a0_hbm, a, in_sem.at[0])

    per_pair = 2 * n_gu // n_d

    def piece(h, n):
        is_gu = (h < a_end) | ((h >= c_end) & (h < a2_end))
        layer, j = jnp.where(h < a_end, last, 0), jnp.where(h < a_end, h + 1, h - c_end)
        i = jnp.where(h < c_end, h - a_end, h - a2_end)
        is_d = ((h >= a_end) & (h < c_end)) | ((h >= a2_end) & (h < c2_end))
        is_da = (h >= a_end) & (h < c_end)

        if n == 0:

            @pl.when(h == c_end)
            def _():
                loop(4, 8, norm_backward)
                a0_load().wait()
                loop(0, 8, transpose_tile)

            pl.when(h == a_end)(lambda: a0_load().start())

        @pl.when(is_gu)
        def _():
            if n == 0:
                wait(weight_loads(layer, j, True))
            if n < HALVES:
                backward_tile(n, j)
            else:
                gu_grads(layer, j, h + 1)

        @pl.when(is_d & (i % 2 == 0))
        def _():
            if n < 2:
                d_grads(n, i // 2, h + 1)

        @pl.when(is_da & (i % 2 == 1))
        def _():
            da_block((i // 2) * per_pair + 1 + n)

        if n == 2:

            @pl.when(is_da & (i % 2 == 0))
            def _():
                da_block((i // 2) * per_pair)

            @pl.when(h == c_end - 1)
            def _():
                loop(0, 4, norm_backward)

    barrier = pltpu.get_barrier_semaphore()
    for f in range(FLOWS):
        pl.semaphore_signal(barrier, inc=1, device_id=on_first(f, 0), device_id_type=MESH)
    half = pl.ds(0, z.tokens // 2), pl.ds(z.tokens // 2, z.tokens // 2)
    x_loads = [pltpu.make_async_copy(x_in.at[half[n]], hb.at[half[n]], in_sem.at[n]) for n in range(2)]
    dy_load = pltpu.make_async_copy(dy_in, d, in_sem.at[0])
    a0_store = pltpu.make_async_copy(a, a0_hbm, in_sem.at[1])
    start(x_loads + weight_loads(0, 0, False))
    for n in range(2):
        x_loads[n].wait()
        loop(4 * n, 4 * n + 4, first_norm)
    start(weight_loads(0, 1, False))
    a0_store.start()
    start(f2_loads(0) + f2_loads(1))
    dy_load.start()
    loop(0, n_gu, f1_block)
    loop(0, z.d // fb, f2_block)
    a0_store.wait()
    loop(0, 8, norm_and_transpose)
    dy_load.wait()
    wait(weight_loads(last, 0, True))
    loop(0, HALVES, lambda t: backward_tile(t, 0))
    gu_grads(last, 0, 0)
    pl.semaphore_wait(barrier, FLOWS)

    def half_step(h):
        slot_0(h)
        piece(h, 0)
        slot_1(h)
        piece(h, 1)
        slot_2(h)
        piece(h, 2)

    loop(0, z.units + 5, half_step)


def train_kernel_call(z, x, dy, weights, moments):
    side, rows, cols, fb = z.side, z.rows, z.cols, z.fb
    dma = pltpu.SemaphoreType.DMA
    hbm = pl.BlockSpec(memory_space=pl.ANY)
    out_shape = (
        jax.ShapeDtypeStruct((z.units, FLOWS, z.group, rows, cols), BF16),
        jax.ShapeDtypeStruct((z.units, FLOWS, rows, cols), BF16),
        jax.ShapeDtypeStruct((z.gu_units, z.tokens, 2 * fb), BF16),
        jax.ShapeDtypeStruct((z.tokens, z.d), BF16),
    )
    scratch = [
        pltpu.VMEM((z.tokens, z.d), BF16),
        pltpu.VMEM((z.d, z.tokens), BF16),
        pltpu.VMEM((z.tokens, z.d), BF16),
        pltpu.VMEM((z.tokens, z.d), BF16),
        pltpu.VMEM((z.tokens, z.d), F32),
        pltpu.VMEM((z.ff, z.tokens), BF16),
        pltpu.VMEM((2, z.d, 2 * fb), BF16),
        pltpu.VMEM((2, fb, z.d), BF16),
        pltpu.VMEM((2, z.tokens, 2 * fb), BF16),
        pltpu.VMEM((SLOTS, FLOWS, z.group, rows, cols), BF16),
        pltpu.VMEM((2, COPIES, FLOWS, side, rows, cols), BF16),
        pltpu.VMEM((2, FLOWS, side, rows, cols), BF16),
        pltpu.VMEM((2, FLOWS, side, rows, cols), F32),
        pltpu.VMEM((2, COPIES, FLOWS, rows, cols), BF16),
        pltpu.VMEM((2, COPIES, FLOWS, rows, cols), BF16),
        pltpu.VMEM((2, FLOWS, rows, cols), BF16),
        pltpu.VMEM((2, FLOWS, rows, cols), BF16),
        pltpu.VMEM((2, FLOWS, rows, cols), BF16),
        pltpu.VMEM((2, FLOWS, rows, cols), F32),
        pltpu.VMEM((2, FLOWS, rows, cols), F32),
        pltpu.VMEM((2, FLOWS, rows, cols), BF16),
        *[dma((n, *two)) for n in (2, 2, SETS, AH_SETS) for two in ((), (2,))],
        dma((2,)),
        dma((2,)),
        dma((2, 3)),
        dma((2, 3)),
        dma((2,)),
        dma((2,)),
        dma((2,)),
        dma((4, 2)),
    ]
    return pl.pallas_call(
        functools.partial(step_kernel, z),
        out_shape=out_shape,
        in_specs=[hbm] * 11,
        out_specs=(hbm,) * 4,
        scratch_shapes=scratch,
        name="train_step",
        compiler_params=pltpu.CompilerParams(collective_id=0, has_side_effects=True, vmem_limit_bytes=VMEM_LIMIT),
    )(x, dy, *weights, *moments)


def unpack_kernel(z, w_all, g_all, *refs):
    side, rows, cols = z.side, z.rows, z.cols
    olds, (wg_out, wu_out, wd_out), news, rest = refs[:6], refs[6:9], refs[9:15], refs[15:]
    gu_buf, d_buf, g_buf, *moments, in_sem, out_sem, g_sem, old_sem, new_sem = rest
    gu_cols, d_cols = 2 * UNPACK * cols, UNPACK * cols
    gu_steps, d_steps = z.gu_steps, z.d_units // UNPACK
    steps = gu_steps + d_steps

    def lanes(at, n):
        return pl.ds(pl.multiple_of(at, n), n)

    def unit_of(n, c, k):
        return (z.layers - 1 - n) * z.per_layer + c * UNPACK + k

    def buffer(c):
        return gu_buf.at[c] if c < gu_steps else d_buf.at[c - gu_steps]

    def fetch(n, c):
        def unit(k):
            u = unit_of(n, c, k)
            for f in range(FLOWS):
                if c < gu_steps:
                    dst = gu_buf.at[c, f // 2, :, :, :, lanes((2 * k + f % 2) * cols, cols)]
                else:
                    dst = d_buf.at[c - gu_steps, :, :, f, :, lanes(k * cols, cols)]
                if f < 2:
                    pltpu.make_async_copy(w_all.at[u, f], dst, in_sem.at[c]).start()
                else:
                    for y in range(side):
                        pltpu.make_async_copy(w_all.at[u, f, y], dst.at[:, y], in_sem.at[c]).start()

        lax.fori_loop(0, UNPACK, lambda k, _: (unit(k), _)[1], 0)

    def stores(n, c):
        if c < gu_steps:
            place = (n, slice(None), slice(None), slice(None), pl.ds(c * gu_cols, gu_cols))
            return [
                pltpu.make_async_copy(gu_buf.at[c, k], out.at[place], out_sem.at[c, k])
                for k, out in enumerate((wg_out, wu_out))
            ]
        place = (n, slice(None), slice(None), slice(None), slice(None), pl.ds((c - gu_steps) * d_cols, d_cols))
        return [pltpu.make_async_copy(d_buf.at[c - gu_steps], wd_out.at[place], out_sem.at[c, 0])]

    def step_moments(n, c):
        def unit(k):
            u = unit_of(n, c, k)
            for f in range(FLOWS):
                g = g_buf[u, f].astype(F32)
                if c < gu_steps:
                    kind, place = f // 2, (n, slice(None), lanes(c * gu_cols + (2 * k + f % 2) * cols, cols))
                else:
                    kind, place = 2, (n, pl.ds(f * rows, rows), lanes((c - gu_steps) * d_cols + k * cols, cols))
                m, v = moments[kind], moments[kind + 3]
                _, m[place], v[place] = adamw(g, m[place], v[place], g)

        lax.fori_loop(0, UNPACK, lambda k, _: (unit(k), _)[1], 0)
        for kind in (0, 1) if c < gu_steps else (2,):
            part = pl.ds(c * gu_cols, gu_cols) if c < gu_steps else pl.ds((c - gu_steps) * d_cols, d_cols)
            for t in (kind, kind + 3):
                pltpu.make_async_copy(moments[t].at[n, :, part], news[t].at[n, :, part], new_sem.at[t]).start()

    for c in range(2):
        fetch(0, c)
    g_load = pltpu.make_async_copy(g_all, g_buf, g_sem)
    old_loads = [pltpu.make_async_copy(olds[t], moments[t], old_sem.at[t]) for t in range(6)]
    for copy in [g_load, *old_loads]:
        copy.start()
    for c in range(2, steps):
        fetch(0, c)

    def layer(n):
        for c in range(steps):
            pltpu.make_async_copy(buffer(c), buffer(c), in_sem.at[c]).wait()
            for copy in stores(n, c):
                copy.start()
            if c == 0:

                @pl.when(n == 0)
                def _():
                    for copy in [g_load, *old_loads]:
                        copy.wait()

            step_moments(n, c)
            for done in ([c - 1] if c else []) + ([c] if c == steps - 1 else []):
                for copy in stores(n, done):
                    copy.wait()
                pl.when(n + 1 < z.layers)(lambda done=done: fetch(n + 1, done))

    lax.fori_loop(0, z.layers, lambda n, _: (layer(n), _)[1], 0)
    for t in range(6):
        pltpu.make_async_copy(moments[t], news[t], new_sem.at[t]).wait()


def unpack(z, w_all, g_all, moments):
    side, rows, cols = z.side, z.rows, z.cols
    dma = pltpu.SemaphoreType.DMA
    hbm = pl.BlockSpec(memory_space=pl.ANY)
    steps = z.per_layer // UNPACK
    grid = (side, side)
    like = [jax.ShapeDtypeStruct(t.shape, t.dtype) for t in moments]
    gate = jax.ShapeDtypeStruct((z.layers, *grid, rows, z.ff), BF16)
    down = jax.ShapeDtypeStruct((z.layers, *grid, FLOWS, rows, z.d), BF16)
    wg, wu, wd, *new = pl.pallas_call(
        functools.partial(unpack_kernel, z),
        in_specs=[hbm] * 8,
        out_specs=(hbm,) * 9,
        out_shape=(gate, gate, down, *like),
        scratch_shapes=[
            pltpu.VMEM((z.gu_steps, 2, *grid, rows, 2 * UNPACK * cols), BF16),
            pltpu.VMEM((z.d_units // UNPACK, *grid, FLOWS, rows, UNPACK * cols), BF16),
            pltpu.VMEM(g_all.shape, BF16),
            *[pltpu.VMEM(t.shape, F32) for t in moments],
            dma((steps,)),
            dma((steps, 2)),
            dma,
            dma((6,)),
            dma((6,)),
        ],
        name="unpack",
        compiler_params=pltpu.CompilerParams(vmem_limit_bytes=VMEM_LIMIT),
    )(w_all.reshape(z.units, FLOWS, *grid, rows, cols), g_all, *moments)
    return wg.reshape(z.layers, z.d, z.ff), wu.reshape(z.layers, z.d, z.ff), wd.reshape(z.layers, z.ff, z.d), *new


def solution(mesh):
    group = mesh.shape["dp"]

    def device_step(x, dy, wg, wu, wd, *moments):
        x, dy = x[0], dy[0]
        z = Sizes(x.shape[0], x.shape[1], wg.shape[2], wg.shape[0], group)
        w_all, g_all, *_ = train_kernel_call(z, x, dy, (wg, wu, wd), moments)
        return unpack(z, w_all, g_all, moments)

    seq, own, part, out = P(("rep", "dp")), P(), P(None, "dp"), P("rep")
    return jax.shard_map(
        device_step,
        mesh=mesh,
        in_specs=(seq, seq, own, own, own, *([part] * 6)),
        out_specs=(out, out, out, *([P("rep", "dp")] * 6)),
        check_vma=False,
    )
```

```python
import functools
import math

import jax
import jax.numpy as jnp
from jax import lax
from jax.experimental import pallas as pl
from jax.experimental.pallas import tpu as pltpu
from jax.sharding import PartitionSpec as P

F32, BF16 = jnp.float32, jnp.bfloat16
MESH = pl.DeviceIdType.MESH
VMEM_LIMIT = 64 * 1024 * 1024 - 128 * 1024
FLOWS = 4
COPIES = 3
UNPACK = 4
LAST = 2
HURRIED = 2
SETS = 4
AH_SETS = 8
SLOTS = 4
HALVES = 2


def mm(a, b, dims=((1,), (0,))):
    return lax.dot_general(a, b, (dims, ((), ())), preferred_element_type=F32)


def scale_of(wide):
    return lax.rsqrt(jnp.mean(wide**2, -1, keepdims=True) + 1e-6)


def adamw(w, m, v, g):
    m = 0.9 * m + 0.1 * g
    v = 0.95 * v + 0.05 * g * g
    step = m * lax.rsqrt(v + 1e-8) + 0.1 * w
    return (w - 0.02 * step).astype(BF16), m, v


class Sizes:
    def __init__(self, tokens, d, ff, layers, group):
        self.tokens, self.d, self.ff, self.layers, self.group = tokens, d, ff, layers, group
        self.side = math.isqrt(group)
        self.rows = d // group
        self.quarters = ff // group // self.rows
        assert self.quarters == FLOWS and self.side == 4
        self.cols = d // 8
        self.fb = 2 * self.cols
        self.gu_units = ff // self.fb
        self.d_units = d // self.cols
        self.per_layer = self.gu_units + self.d_units
        self.units = layers * self.per_layer
        self.gu_steps = self.gu_units // UNPACK
        self.pieces = ff // d
        assert layers == 2 and ff == 2 * tokens and tokens == 2 * d and self.fb * self.pieces == d


def step_kernel(
    z,
    x_in, dy_in, wg_in, wu_in, wd_in, mg_in, mu_in, md_in, vg_in, vu_in, vd_in,
    w_out, g_out, dgu_hbm, a0_hbm,
    a, at, d, hb, da, big, wgu, wd, dgu, grads,
    hrecv, hsend, hsum, lrecv, lsend, w_new, g_own, w_old, m_old, v_old, lx,
    hs, hr, ls, lr, als, alr, ahs, ahr, own_sem, g_sem, adam_sem, w_sem, in_sem, dgu_sem, f_sem, x_sem,
):
    side, rows, cols, fb = z.side, z.rows, z.cols, z.fb
    rep, me = lax.axis_index("rep"), lax.axis_index("dp")
    cx, cy = me // side, me % side
    first = [cx, cx, cy, cy]
    second = [cy, cy, cx, cx]
    way = [1, -1, 1, -1]

    def device(x, y):
        return (rep, ((x + side) % side) * side + (y + side) % side)

    def on_first(f, s):
        n = way[f] * (-1 if s == 1 else 1)
        return device(cx + n, cy) if f < 2 else device(cx, cy + n)

    def on_second(f, s, far=1):
        n = way[f] * (-1 if s == 1 else far)
        return device(cx, cy + n) if f < 2 else device(cx + n, cy)

    def behind(at_, f, n):
        return (at_ - way[f] * n + 2 * side) % side

    def remote(src, dst, send, recv, target):
        return pltpu.make_async_remote_copy(src, dst, send, recv, device_id=target, device_id_type=MESH)

    def h_copy(u, s, f):
        par = u % 2
        src = hsend.at[par, f] if s == 2 else grads.at[u % SLOTS, f, pl.ds(side * behind(first[f], f, 2 - s), side)]
        return remote(src, hrecv.at[par, s, f], hs.at[par], hr.at[par, (s + 1) // 2], on_first(f, s))

    def l_copy(u, s, f):
        par = u % 2
        return remote(lsend.at[par, s, f], lrecv.at[par, s, f], ls.at[par], lr.at[par, (s + 1) // 2], on_second(f, s))

    def al_copy(u, s, f):
        k = u % SETS
        dst = w_out.at[u, f, side * first[f] + behind(second[f], f, s // 2)]
        return remote(w_new.at[u % 2, f] if s < 2 else dst, dst, als.at[k], alr.at[k, (s + 1) // 2], on_second(f, s))

    def ah_copy(u, s, f):
        k = u % AH_SETS
        dst = w_out.at[u, f, pl.ds(side * behind(first[f], f, s // 2), side)]
        return remote(dst, dst, ahs.at[k], ahr.at[k, (s + 1) // 2], on_first(f, s))

    def own_copy(u, f):
        return pltpu.make_async_copy(w_new.at[u % 2, f], w_out.at[u, f, side * first[f] + second[f]], own_sem.at[u % 2])

    def wait_for(copies, big, sem):
        size = (hrecv if big else lrecv).at[0, pl.ds(0, copies)]
        pltpu.make_async_copy(size, size, sem).wait()

    def g_copy(u):
        return pltpu.make_async_copy(g_own.at[u % 2], g_out.at[u], g_sem.at[u % 2])

    def place_of(u):
        return z.layers - 1 - u // z.per_layer, u % z.per_layer

    def adam_loads(u, start):
        layer, k = place_of(u)
        par = u % 2

        def go(copies):
            for c in copies:
                c.start()

        def copies_gu():
            c0 = pl.multiple_of(k * fb, fb)
            r0 = pl.multiple_of(me * rows, rows)
            out = []
            for f in range(FLOWS):
                col = pl.ds(c0 + (f % 2) * cols, cols)
                w_, m_, v_ = ((wg_in, mg_in, vg_in), (wu_in, mu_in, vu_in))[f // 2]
                out.append(pltpu.make_async_copy(w_.at[layer, pl.ds(r0, rows), col], w_old.at[par, f], adam_sem.at[par, 0]))
                out.append(pltpu.make_async_copy(m_.at[layer, :, col], m_old.at[par, f], adam_sem.at[par, 1]))
                out.append(pltpu.make_async_copy(v_.at[layer, :, col], v_old.at[par, f], adam_sem.at[par, 2]))
            return out

        def copies_d():
            col = pl.ds(pl.multiple_of((k - z.gu_units) * cols, cols), cols)
            out = []
            for f in range(FLOWS):
                r0 = pl.multiple_of((me * FLOWS + f) * rows, rows)
                out.append(pltpu.make_async_copy(wd_in.at[layer, pl.ds(r0, rows), col], w_old.at[par, f], adam_sem.at[par, 0]))
                out.append(pltpu.make_async_copy(md_in.at[layer, pl.ds(f * rows, rows), col], m_old.at[par, f], adam_sem.at[par, 1]))
                out.append(pltpu.make_async_copy(vd_in.at[layer, pl.ds(f * rows, rows), col], v_old.at[par, f], adam_sem.at[par, 2]))
            return out

        if start:
            pl.when(k < z.gu_units)(lambda: go(copies_gu()))
            pl.when(k >= z.gu_units)(lambda: go(copies_d()))
        else:
            for n, old in enumerate((w_old, m_old, v_old)):
                pltpu.make_async_copy(old.at[par], old.at[par], adam_sem.at[par, n]).wait()

    def start(copies):
        for c in copies:
            c.start()

    def wait(copies):
        for c in copies:
            c.wait()

    def both(x, y):
        return x.astype(F32) + y.astype(F32)

    flows = range(FLOWS)

    def group(f, n):
        return pl.ds(side * behind(first[f], f, n), side)

    def h_a(u):
        for f in flows:
            start([h_copy(u, 0, f), h_copy(u, 1, f)])

    def h_b(u):
        par = u % 2
        wait_for(1, True, hr.at[par, 0])
        for f in flows:
            hsend[par, f] = both(hrecv[par, 0, f], grads[u % SLOTS, f, group(f, 3)]).astype(BF16)
        for f in flows:
            h_copy(u, 2, f).start()

    def h_end(u):
        par = u % 2
        wait_for(2, True, hr.at[par, 1])
        for f in flows:
            hsum[par, f] = both(hrecv[par, 1, f], hrecv[par, 2, f]) + grads[u % SLOTS, f, group(f, 0)].astype(F32)

    def l_a(u):
        par = u % 2
        h_end(u)
        for f in flows:
            for s in range(2):
                lsend[par, s, f] = hsum[par, f, behind(second[f], f, 2 - s)].astype(BF16)
        for f in flows:
            start([l_copy(u, 0, f), l_copy(u, 1, f)])
        wait_for(COPIES, True, hs.at[par])

    def step_weight(u, f, total):
        par, g = u % 2, total.astype(BF16)
        g_own[par, f] = g
        w_new[par, f] = adamw(w_old[par, f].astype(F32), m_old[par, f], v_old[par, f], g.astype(F32))[0]

    def l_b(u):
        par = u % 2
        wait_for(1, False, lr.at[par, 0])
        for f in flows:
            lsend[par, 2, f] = both(lrecv[par, 0, f], hsum[par, f, behind(second[f], f, 3)]).astype(BF16)
        for f in flows:
            l_copy(u, 2, f).start()

    def al_a(u):
        par = u % 2
        adam_loads(u, False)
        wait_for(2, False, lr.at[par, 1])
        for f in flows:
            step_weight(u, f, both(lrecv[par, 1, f], lrecv[par, 2, f]) + hsum[par, f, second[f]])
        for f in flows:
            start([al_copy(u, 0, f), al_copy(u, 1, f), own_copy(u, f)])
        g_copy(u).start()
        wait_for(COPIES, False, ls.at[par])

    def al_b(u):
        wait_for(1, False, alr.at[u % SETS, 0])
        for f in flows:
            al_copy(u, 2, f).start()

    def al_end(u):
        wait_for(2, False, alr.at[u % SETS, 1])
        wait_for(COPIES, False, als.at[u % SETS])
        wait_for(1, False, own_sem.at[u % 2])
        g_copy(u).wait()

    def ah_a(u):
        for f in flows:
            start([ah_copy(u, 0, f), ah_copy(u, 1, f)])

    def ah_b(u):
        wait_for(1, True, ahr.at[u % AH_SETS, 0])
        for f in flows:
            ah_copy(u, 2, f).start()

    def ah_end(u):
        wait_for(2, True, ahr.at[u % AH_SETS, 1])
        wait_for(COPIES, True, ahs.at[u % AH_SETS])

    def if_unit(u, step, lo=0, hi=z.units):
        pl.when((u >= lo) & (u < hi))(lambda: step(u))

    def l_last(u, f):
        return remote(lsend.at[u % 2, 2, f], lx.at[u % 2, f], x_sem.at[0, u % 2], x_sem.at[1, u % 2], on_second(f, 2, 2))

    def al_last(u, s, f):
        if s < 2:
            return al_copy(u, s, f)
        dst = w_out.at[u, f, side * first[f] + second[f]]
        return remote(w_new.at[u % 2, f], dst, x_sem.at[2, u % 2], x_sem.at[3, u % 2], on_second(f, 2, 2))

    def wait_for_last(u, send, recv, far):
        wait_for(1, False, recv.at[0])
        wait_for(1, False, recv.at[1])
        wait_for(1, False, x_sem.at[far + 1, u % 2])
        wait_for(2, False, send)
        wait_for(1, False, x_sem.at[far, u % 2])

    def l_a_last(u):
        h_end(u)
        par = u % 2
        for f in flows:
            for s, n in enumerate((3, 1, 2)):
                lsend[par, s, f] = hsum[par, f, behind(second[f], f, n)].astype(BF16)
        for f in flows:
            start([l_copy(u, 0, f), l_copy(u, 1, f), l_last(u, f)])
        wait_for(COPIES, True, hs.at[par])

    def al_a_last(u):
        par = u % 2
        adam_loads(u, False)
        wait_for_last(u, ls.at[par], lr.at[par], 0)
        for f in flows:
            step_weight(u, f, both(lrecv[par, 0, f], lrecv[par, 1, f]) + both(lx[par, f], hsum[par, f, second[f]]))
        for f in flows:
            start([al_last(u, s, f) for s in range(COPIES)] + [own_copy(u, f)])
        g_copy(u).start()

    def ah_a_last(u):
        wait_for_last(u, als.at[u % SETS], alr.at[u % SETS], 2)
        wait_for(1, False, own_sem.at[u % 2])
        ah_a(u)
        g_copy(u).wait()

    last_ones = z.units - LAST
    hurried = last_ones - HURRIED

    def slot_0(h):
        if_unit(h - 2, l_b, 0, last_ones)
        if_unit(h, h_a)
        if_unit(h - 4, al_end, hurried, last_ones)
        if_unit(h - 4, ah_a, hurried, last_ones)
        if_unit(h - 2, al_a_last, last_ones)
        if_unit(h - 4, ah_end, last_ones)

    def slot_1(h):
        if_unit(h - 3, al_b, 0, last_ones)
        if_unit(h - 1, l_a, 0, last_ones)
        if_unit(h - 1, l_a_last, last_ones)
        if_unit(h - 6, ah_end, 0, hurried)
        if_unit(h - 5, ah_end, hurried, last_ones)
        if_unit(h - 4, al_end, 0, hurried)
        if_unit(h - 4, ah_a, 0, hurried)
        if_unit(h - 3, ah_b, last_ones)
        if_unit(h - 1, lambda u: adam_loads(u, True))

    def slot_2(h):
        if_unit(h, h_b)
        if_unit(h - 2, al_a, 0, last_ones)
        if_unit(h - 5, ah_b, 0, hurried)
        if_unit(h - 4, ah_b, hurried, last_ones)
        if_unit(h - 2, ah_a_last, last_ones)

    tile = z.tokens // HALVES
    last = z.layers - 1
    n_gu, n_d = z.gu_units, z.d_units
    a_end = n_gu - 1
    c_end = a_end + n_d
    a2_end = c_end + n_gu
    c2_end = a2_end + n_d
    wide_tile = z.tokens // 8

    def rows_of(t, size):
        return pl.ds(pl.multiple_of(t * size, size), size)

    def loop(lo, hi, body):
        lax.fori_loop(lo, hi, lambda i, c: (body(i), c)[1], 0)

    def weight_loads(layer, j, with_down):
        buf, cols_j = j % 2, rows_of(j, fb)
        out = [
            pltpu.make_async_copy(wg_in.at[layer, :, cols_j], wgu.at[buf, :, pl.ds(0, fb)], w_sem.at[buf, 0]),
            pltpu.make_async_copy(wu_in.at[layer, :, cols_j], wgu.at[buf, :, pl.ds(fb, fb)], w_sem.at[buf, 1]),
        ]
        if with_down:
            out.append(pltpu.make_async_copy(wd_in.at[layer, cols_j, :], wd.at[buf], w_sem.at[buf, 2]))
        return out

    def dgu_load(j):
        return pltpu.make_async_copy(dgu_hbm.at[j], dgu.at[j % 2], dgu_sem.at[j % 2])

    def dgu_store(j):
        return pltpu.make_async_copy(dgu.at[j % 2], dgu_hbm.at[j], dgu_sem.at[j % 2])

    def normed_of(wide):
        return (wide * scale_of(wide)).astype(BF16)

    def f1_block(j):
        wait(weight_loads(0, j, False))
        gu = mm(a[...], wgu[j % 2])
        gate, up = gu[:, :fb], gu[:, fb:]
        c0 = j * fb
        big[rows_of(c0 // z.tokens, z.tokens), pl.ds(pl.multiple_of(c0 % z.tokens, fb), fb)] = (jax.nn.silu(gate) * up).astype(BF16)
        pl.when(j + 2 < n_gu)(lambda: start(weight_loads(0, j + 2, False)))
        pl.when(j + 2 >= n_gu)(lambda: start(weight_loads(last, j + 2 - n_gu, True)))

    def f2_loads(n):
        buf = n % 2
        out = []
        for k in range(z.pieces):
            dst = at.at[:, pl.ds(pl.multiple_of(buf * d_half + k * fb, fb), fb)]
            out.append(pltpu.make_async_copy(wd_in.at[0, pl.ds(k * z.d, z.d), rows_of(n, fb)], dst, f_sem.at[buf]))
        return out

    d_half = z.tokens // 2

    def f2_block(n):
        both_k = at.at[:, pl.ds(0, d_half)]
        pltpu.make_async_copy(both_k, both_k, f_sem.at[n % 2]).wait()

        def part(t):
            acc = None
            for k in range(z.pieces):
                r = pl.ds(pl.multiple_of((k // 2) * z.tokens + t * tile, tile), tile)
                w_k = at[:, pl.ds(pl.multiple_of((n % 2) * d_half + k * fb, fb), fb)]
                one = mm(big[r, pl.ds((k % 2) * z.d, z.d)], w_k)
                acc = one if acc is None else acc + one
            here = (rows_of(t, tile), rows_of(n, fb))
            hb[here] = both(hb[here], acc.astype(BF16)).astype(BF16)

        loop(0, HALVES, part)
        pl.when(n + 2 < z.d // fb)(lambda: start(f2_loads(n + 2)))

    def first_norm(t):
        r = rows_of(t, wide_tile)
        a[r, :] = normed_of(hb[r, :].astype(F32))

    def second_norm(t):
        r = rows_of(t, wide_tile)
        a[r, :] = normed_of(hb[r, :].astype(F32))

    def transpose_tile(t):
        r = rows_of(t, wide_tile)
        at[:, r] = a[r, :].T

    def backward_tile(t, j, transpose=False):
        buf, r = j % 2, rows_of(t, tile)
        if transpose:
            at[:, r] = a[r, :].T
        gu = mm(a[r, :], wgu[buf])
        gate, up = gu[:, :fb], gu[:, fb:]
        dp = mm(d[r, :], wd[buf], ((1,), (1,))).astype(BF16).astype(F32)
        sig = jax.nn.sigmoid(gate)
        silu = gate * sig
        big[rows_of(j, fb), r] = (silu * up).astype(BF16).T
        dgu[buf, r, pl.ds(fb, fb)] = (dp * silu).astype(BF16)
        dgu[buf, r, pl.ds(0, fb)] = (dp * up * (sig * (1 + gate * (1 - sig)))).astype(BF16)

    def store_block(slot, f, dev, value):
        x, y = dev // side, dev % side
        grads[slot, f, x * side + y if f < 2 else y * side + x] = value

    def gu_grads(layer, j, u):
        pl.when(layer == last)(lambda: dgu_store(j).start())
        out = mm(at[...], dgu[j % 2]).astype(BF16)
        for dev in range(z.group):
            for f in range(FLOWS):
                store_block(u % SLOTS, f, dev, out[dev * rows : (dev + 1) * rows, f * cols : (f + 1) * cols])

        @pl.when(layer == last)
        def _():
            dgu_store(j).wait()

            @pl.when(j + 2 < n_gu)
            def _():
                start(weight_loads(last, j + 2, True))

            @pl.when(j + 2 >= n_gu)
            def _():
                start(weight_loads(last, j + 2 - n_gu, False))
                dgu_load(j + 2 - n_gu).start()

        pl.when((layer != last) & (j + 2 < n_gu))(lambda: start(weight_loads(0, j + 2, True)))

    def d_grads(t, pair, u):
        devices = z.group // 2
        out = mm(big[rows_of(t, z.ff // 2), :], d[:, rows_of(pair, 2 * cols)]).astype(BF16)
        for n in range(devices):
            for f in range(FLOWS):
                r0 = (n * FLOWS + f) * rows
                for k in range(2):
                    store_block((u + k) % SLOTS, f, t * devices + n, out[r0 : r0 + rows, k * cols : (k + 1) * cols])

    def da_block(k):
        buf = k % 2
        wait(weight_loads(last, k, False))
        dgu_load(k).wait()

        def part(t, first):
            r = rows_of(t, tile)
            new = mm(dgu[buf, r, :], wgu[buf], ((1,), (1,)))
            da[r, :] = new if first else da[r, :] + new

        pl.when(k == 0)(lambda: loop(0, HALVES, lambda t: part(t, True)))
        pl.when(k != 0)(lambda: loop(0, HALVES, lambda t: part(t, False)))

        @pl.when(k + 2 < n_gu)
        def _():
            start(weight_loads(last, k + 2, False))
            dgu_load(k + 2).start()

        pl.when(k + 2 >= n_gu)(lambda: start(weight_loads(0, k + 2 - n_gu, True)))

    def norm_backward(t):
        r = rows_of(t, wide_tile)
        wide = hb[r, :].astype(F32)
        scale = scale_of(wide)
        by_a = da[r, :].astype(BF16).astype(F32)
        inner = jnp.mean(by_a * wide, -1, keepdims=True)
        d[r, :] = both(d[r, :], (scale * by_a - wide * (scale**3 * inner)).astype(BF16)).astype(BF16)

    def a0_load():
        return pltpu.make_async_copy(a0_hbm, a, in_sem.at[0])

    per_pair = 2 * n_gu // n_d

    def piece(h, n):
        is_gu = (h < a_end) | ((h >= c_end) & (h < a2_end))
        layer, j = jnp.where(h < a_end, last, 0), jnp.where(h < a_end, h + 1, h - c_end)
        i = jnp.where(h < c_end, h - a_end, h - a2_end)
        is_d = ((h >= a_end) & (h < c_end)) | ((h >= a2_end) & (h < c2_end))
        is_da = (h >= a_end) & (h < c_end)

        if n == 0:

            @pl.when(h == c_end)
            def _():
                a0_load().wait()
                loop(0, 8, transpose_tile)

            pl.when(h == a_end)(lambda: a0_load().start())

        @pl.when(is_gu)
        def _():
            if n == 0:
                wait(weight_loads(layer, j, True))
            if n < HALVES:
                backward_tile(n, j)
            else:
                gu_grads(layer, j, h + 1)

        @pl.when(is_d & (i % 2 == 0))
        def _():
            if n < 2:
                d_grads(n, i // 2, h + 1)

        @pl.when(is_da)
        def _():
            odd, later = i % 2, jnp.where(i > 1, 1, 0)
            lo = jnp.where(odd == 1, (i // 2) * per_pair + 1 + n + later, (i // 2) * per_pair + later)
            count = odd if n < 2 else 1 + jnp.where(i == 1, 1, 0)
            loop(lo, jnp.minimum(lo + count, n_gu), da_block)

        if n == 2:

            @pl.when(h == c_end - 1)
            def _():
                loop(0, 8, norm_backward)

    barrier = pltpu.get_barrier_semaphore()
    for f in range(FLOWS):
        pl.semaphore_signal(barrier, inc=1, device_id=on_first(f, 0), device_id_type=MESH)
    half = pl.ds(0, z.tokens // 2), pl.ds(z.tokens // 2, z.tokens // 2)
    x_loads = [pltpu.make_async_copy(x_in.at[half[n]], hb.at[half[n]], in_sem.at[n]) for n in range(2)]
    dy_load = pltpu.make_async_copy(dy_in, d, in_sem.at[0])
    a0_store = pltpu.make_async_copy(a, a0_hbm, in_sem.at[1])
    start(x_loads + weight_loads(0, 0, False))
    for n in range(2):
        x_loads[n].wait()
        loop(4 * n, 4 * n + 4, first_norm)
    start(weight_loads(0, 1, False))
    a0_store.start()
    start(f2_loads(0) + f2_loads(1))
    dy_load.start()
    loop(0, n_gu, f1_block)
    loop(0, z.d // fb, f2_block)
    a0_store.wait()
    loop(0, 8, second_norm)
    dy_load.wait()
    wait(weight_loads(last, 0, True))
    loop(0, HALVES, lambda t: backward_tile(t, 0, True))
    gu_grads(last, 0, 0)
    pl.semaphore_wait(barrier, FLOWS)

    def half_step(h):
        slot_0(h)
        piece(h, 0)
        slot_1(h)
        piece(h, 1)
        slot_2(h)
        piece(h, 2)

    loop(0, z.units + 5, half_step)


def train_kernel_call(z, x, dy, weights, moments):
    side, rows, cols, fb = z.side, z.rows, z.cols, z.fb
    dma = pltpu.SemaphoreType.DMA
    hbm = pl.BlockSpec(memory_space=pl.ANY)
    out_shape = (
        jax.ShapeDtypeStruct((z.units, FLOWS, z.group, rows, cols), BF16),
        jax.ShapeDtypeStruct((z.units, FLOWS, rows, cols), BF16),
        jax.ShapeDtypeStruct((z.gu_units, z.tokens, 2 * fb), BF16),
        jax.ShapeDtypeStruct((z.tokens, z.d), BF16),
    )
    scratch = [
        pltpu.VMEM((z.tokens, z.d), BF16),
        pltpu.VMEM((z.d, z.tokens), BF16),
        pltpu.VMEM((z.tokens, z.d), BF16),
        pltpu.VMEM((z.tokens, z.d), BF16),
        pltpu.VMEM((z.tokens, z.d), F32),
        pltpu.VMEM((z.ff, z.tokens), BF16),
        pltpu.VMEM((2, z.d, 2 * fb), BF16),
        pltpu.VMEM((2, fb, z.d), BF16),
        pltpu.VMEM((2, z.tokens, 2 * fb), BF16),
        pltpu.VMEM((SLOTS, FLOWS, z.group, rows, cols), BF16),
        pltpu.VMEM((2, COPIES, FLOWS, side, rows, cols), BF16),
        pltpu.VMEM((2, FLOWS, side, rows, cols), BF16),
        pltpu.VMEM((2, FLOWS, side, rows, cols), F32),
        pltpu.VMEM((2, COPIES, FLOWS, rows, cols), BF16),
        pltpu.VMEM((2, COPIES, FLOWS, rows, cols), BF16),
        pltpu.VMEM((2, FLOWS, rows, cols), BF16),
        pltpu.VMEM((2, FLOWS, rows, cols), BF16),
        pltpu.VMEM((2, FLOWS, rows, cols), BF16),
        pltpu.VMEM((2, FLOWS, rows, cols), F32),
        pltpu.VMEM((2, FLOWS, rows, cols), F32),
        pltpu.VMEM((2, FLOWS, rows, cols), BF16),
        *[dma((n, *two)) for n in (2, 2, SETS, AH_SETS) for two in ((), (2,))],
        dma((2,)),
        dma((2,)),
        dma((2, 3)),
        dma((2, 3)),
        dma((2,)),
        dma((2,)),
        dma((2,)),
        dma((4, 2)),
    ]
    return pl.pallas_call(
        functools.partial(step_kernel, z),
        out_shape=out_shape,
        in_specs=[hbm] * 11,
        out_specs=(hbm,) * 4,
        scratch_shapes=scratch,
        name="train_step",
        compiler_params=pltpu.CompilerParams(collective_id=0, has_side_effects=True, vmem_limit_bytes=VMEM_LIMIT),
    )(x, dy, *weights, *moments)


def unpack_kernel(z, w_all, g_all, *refs):
    side, rows, cols = z.side, z.rows, z.cols
    olds, (wg_out, wu_out, wd_out), news, rest = refs[:6], refs[6:9], refs[9:15], refs[15:]
    gu_buf, d_buf, g_buf, *moments, in_sem, out_sem, g_sem, old_sem, new_sem = rest
    gu_cols, d_cols = 2 * UNPACK * cols, UNPACK * cols
    gu_steps, d_steps = z.gu_steps, z.d_units // UNPACK
    steps = gu_steps + d_steps

    def lanes(at, n):
        return pl.ds(pl.multiple_of(at, n), n)

    def unit_of(n, c, k):
        return (z.layers - 1 - n) * z.per_layer + c * UNPACK + k

    def buffer(c):
        return gu_buf.at[c] if c < gu_steps else d_buf.at[c - gu_steps]

    def fetch(n, c):
        def unit(k):
            u = unit_of(n, c, k)
            for f in range(FLOWS):
                if c < gu_steps:
                    dst = gu_buf.at[c, f // 2, :, :, :, lanes((2 * k + f % 2) * cols, cols)]
                else:
                    dst = d_buf.at[c - gu_steps, :, :, f, :, lanes(k * cols, cols)]
                if f < 2:
                    pltpu.make_async_copy(w_all.at[u, f], dst, in_sem.at[c]).start()
                else:
                    for y in range(side):
                        pltpu.make_async_copy(w_all.at[u, f, y], dst.at[:, y], in_sem.at[c]).start()

        lax.fori_loop(0, UNPACK, lambda k, _: (unit(k), _)[1], 0)

    def stores(n, c):
        if c < gu_steps:
            place = (n, slice(None), slice(None), slice(None), pl.ds(c * gu_cols, gu_cols))
            return [
                pltpu.make_async_copy(gu_buf.at[c, k], out.at[place], out_sem.at[c, k])
                for k, out in enumerate((wg_out, wu_out))
            ]
        place = (n, slice(None), slice(None), slice(None), slice(None), pl.ds((c - gu_steps) * d_cols, d_cols))
        return [pltpu.make_async_copy(d_buf.at[c - gu_steps], wd_out.at[place], out_sem.at[c, 0])]

    def step_moments(n, c):
        def unit(k):
            u = unit_of(n, c, k)
            for f in range(FLOWS):
                g = g_buf[u, f].astype(F32)
                if c < gu_steps:
                    kind, place = f // 2, (n, slice(None), lanes(c * gu_cols + (2 * k + f % 2) * cols, cols))
                else:
                    kind, place = 2, (n, pl.ds(f * rows, rows), lanes((c - gu_steps) * d_cols + k * cols, cols))
                m, v = moments[kind], moments[kind + 3]
                _, m[place], v[place] = adamw(g, m[place], v[place], g)

        lax.fori_loop(0, UNPACK, lambda k, _: (unit(k), _)[1], 0)
        for kind in (0, 1) if c < gu_steps else (2,):
            part = pl.ds(c * gu_cols, gu_cols) if c < gu_steps else pl.ds((c - gu_steps) * d_cols, d_cols)
            for t in (kind, kind + 3):
                pltpu.make_async_copy(moments[t].at[n, :, part], news[t].at[n, :, part], new_sem.at[t]).start()

    for c in range(2):
        fetch(0, c)
    g_load = pltpu.make_async_copy(g_all, g_buf, g_sem)
    old_loads = [pltpu.make_async_copy(olds[t], moments[t], old_sem.at[t]) for t in range(6)]
    for copy in [g_load, *old_loads]:
        copy.start()
    for c in range(2, steps):
        fetch(0, c)

    def layer(n):
        for c in range(steps):
            pltpu.make_async_copy(buffer(c), buffer(c), in_sem.at[c]).wait()
            for copy in stores(n, c):
                copy.start()
            if c == 0:

                @pl.when(n == 0)
                def _():
                    for copy in [g_load, *old_loads]:
                        copy.wait()

            step_moments(n, c)
            for done in ([c - 1] if c else []) + ([c] if c == steps - 1 else []):
                for copy in stores(n, done):
                    copy.wait()
                pl.when(n + 1 < z.layers)(lambda done=done: fetch(n + 1, done))

    lax.fori_loop(0, z.layers, lambda n, _: (layer(n), _)[1], 0)
    for t in range(6):
        pltpu.make_async_copy(moments[t], news[t], new_sem.at[t]).wait()


def unpack(z, w_all, g_all, moments):
    side, rows, cols = z.side, z.rows, z.cols
    dma = pltpu.SemaphoreType.DMA
    hbm = pl.BlockSpec(memory_space=pl.ANY)
    steps = z.per_layer // UNPACK
    grid = (side, side)
    like = [jax.ShapeDtypeStruct(t.shape, t.dtype) for t in moments]
    gate = jax.ShapeDtypeStruct((z.layers, *grid, rows, z.ff), BF16)
    down = jax.ShapeDtypeStruct((z.layers, *grid, FLOWS, rows, z.d), BF16)
    wg, wu, wd, *new = pl.pallas_call(
        functools.partial(unpack_kernel, z),
        in_specs=[hbm] * 8,
        out_specs=(hbm,) * 9,
        out_shape=(gate, gate, down, *like),
        scratch_shapes=[
            pltpu.VMEM((z.gu_steps, 2, *grid, rows, 2 * UNPACK * cols), BF16),
            pltpu.VMEM((z.d_units // UNPACK, *grid, FLOWS, rows, UNPACK * cols), BF16),
            pltpu.VMEM(g_all.shape, BF16),
            *[pltpu.VMEM(t.shape, F32) for t in moments],
            dma((steps,)),
            dma((steps, 2)),
            dma,
            dma((6,)),
            dma((6,)),
        ],
        name="unpack",
        compiler_params=pltpu.CompilerParams(vmem_limit_bytes=VMEM_LIMIT),
    )(w_all.reshape(z.units, FLOWS, *grid, rows, cols), g_all, *moments)
    return wg.reshape(z.layers, z.d, z.ff), wu.reshape(z.layers, z.d, z.ff), wd.reshape(z.layers, z.ff, z.d), *new


def solution(mesh):
    group = mesh.shape["dp"]

    def device_step(x, dy, wg, wu, wd, *moments):
        x, dy = x[0], dy[0]
        z = Sizes(x.shape[0], x.shape[1], wg.shape[2], wg.shape[0], group)
        w_all, g_all, *_ = train_kernel_call(z, x, dy, (wg, wu, wd), moments)
        return unpack(z, w_all, g_all, moments)

    seq, own, part, out = P(("rep", "dp")), P(), P(None, "dp"), P("rep")
    return jax.shard_map(
        device_step,
        mesh=mesh,
        in_specs=(seq, seq, own, own, own, *([part] * 6)),
        out_specs=(out, out, out, *([P("rep", "dp")] * 6)),
        check_vma=False,
    )
```
